32 devices in a mesh: dp: 8 (over z, core), mp: 4 (over y, x).
Axes of the slice: x: 2, y: 2, z: 4, core: 2. Of those that a mesh axis runs over, the one named last changes fastest.
Arguments:
- token_ids: int32 [8192], P('dp'), may hold values from 0 to 128255
- lengths: int32 [64], P('dp'), may hold values from 1 to 128
- embed_grads: bfloat16 [8192, 4096], P('dp', 'mp'), may hold values from -6 to 6
- vocab_basis: bfloat16 [128256, 32], P('mp'), may hold values from -6 to 6
- embed_basis: bfloat16 [4096, 32], P('mp'), may hold values from -0.09375 to 0.09375
- layer_inputs: bfloat16 [1, 8192, 4096], P(None, 'dp', 'mp'), may hold values from -6 to 6
- layer_grads: bfloat16 [1, 8192, 4096], P(None, 'dp', 'mp'), may hold values from -6 to 6
- input_basis: bfloat16 [1, 4096, 32], P(None, 'mp'), may hold values from -0.09375 to 0.09375
- output_basis: bfloat16 [1, 4096, 32], P(None, 'mp'), may hold values from -0.09375 to 0.09375
- queries: bfloat16 [2, 1024, 256], P(None, 'mp', 'dp'), may hold values from -0.19921875 to 0.19921875
Outputs:
- scores: float32 [64, 256], P('dp')
The draws below stay inside these ranges and needn't reach their ends.
All inputs are finite; a program needn't handle non-finite values.
Results may differ from the reference program's by a relative error of at most 0.0003.
Values may be sent and summed in bfloat16 or wider, within the bound.
No kernel may reach another device: no remote copies, remote signals or barrier semaphores. Data moves between devices by JAX's collectives and lax.ppermute only.
A program may use at most 64 MiB of HBM per device.

```python
import math
import jax
import jax.numpy as jnp
import numpy as np
from jax import lax

D = 4096
VOCAB = 128256
RANK = 32
LIN = 1
SLOT = 128
QUERIES = 256
ITERS = 2
NL = 2
SK = 1024
TOKENS = 8192
EXAMPLES = 64


def set_ends(entries, stream_key, smallest, largest):
    extent = entries.shape
    index_at = [jax.random.randint(jax.random.fold_in(stream_key, axis), (), 0, extent[axis]) for axis in range(len(extent))]
    entries = entries.at[tuple(index_at)].set(smallest)
    longest = extent.index(max(extent))
    index_at[longest] = (index_at[longest] + 1) % extent[longest]
    return entries.at[tuple(index_at)].set(largest)


def block_scale(rng, extent, pieces, low, top_value):
    def one(dim, blocks):
        draws = jax.random.uniform(jax.random.fold_in(jax.random.fold_in(rng, 6), dim), (blocks,), jnp.float32, low / len(pieces), top_value / len(pieces))
        return jnp.repeat(jnp.exp(draws), extent[dim] // blocks).reshape((-1,) + (1,) * (len(extent) - dim - 1))

    loudness = one(*pieces[0])
    for cut in pieces[1:]:
        loudness = loudness * one(*cut)
    return loudness


def ranked_wide(rng, extent, number_of, skew):
    weights = [min(1 << octave, number_of + 1 - (1 << octave)) * (1 << 20) // math.isqrt((1 << octave) ** skew) + 1 for octave in range((number_of + 1).bit_length()) if 1 << octave <= number_of]
    scale = 1 + sum(weights) // (1 << 30)
    listing = np.cumsum(np.array([max(1, weight // scale) for weight in weights]))
    ticket = jax.random.randint(jax.random.fold_in(rng, 1), extent, 0, int(listing[len(weights) - 1]))
    start = jnp.left_shift(1, jnp.searchsorted(jnp.asarray(listing, jnp.int32), ticket, side="right").astype(jnp.int32))
    rank = start - 1 + jax.random.randint(jax.random.fold_in(rng, 4), extent, 0, 1 << 30) % jnp.minimum(start, number_of + 1 - start)
    return jax.random.permutation(jax.random.fold_in(rng, 2), number_of)[rank].astype(jnp.int32)


def normal_values(own_key, shape, scale, bound, pieces=(), kind=jnp.bfloat16):
    gain = block_scale(own_key, shape, pieces, -0.22, 0.18) if pieces else 1.0
    array = jax.random.normal(own_key, shape, jnp.float32) * scale * gain
    return jnp.minimum(jnp.maximum(array, -bound), bound).astype(kind)


def setup_inputs(seed: int = 0) -> dict:
    splits = jax.random.split(jax.random.key(seed), 11)
    token_ids = set_ends(ranked_wide(splits[0], (TOKENS,), VOCAB, 2), jax.random.fold_in(splits[0], 3), 0, VOCAB - 1).astype(jnp.int32)
    lengths = set_ends(jax.random.randint(splits[1], (EXAMPLES,), 1, SLOT + 1), jax.random.fold_in(splits[1], 1), 1, SLOT).astype(jnp.int32)
    embed_grads = normal_values(splits[2], (TOKENS, D), 1.0, 6.0, ((0, 8), (1, 4)))
    vocab_basis = normal_values(splits[3], (VOCAB, RANK), 1.0, 6.0, ((0, 4),))
    embed_basis = normal_values(splits[4], (D, RANK), D ** -0.5, 0.09375, ((0, 4),))
    layer_inputs = normal_values(splits[5], (LIN, TOKENS, D), 1.0, 6.0, ((1, 8), (2, 4)))
    layer_grads = normal_values(splits[6], (LIN, TOKENS, D), 1.0, 6.0, ((1, 8), (2, 4)))
    input_basis = normal_values(splits[7], (LIN, D, RANK), D ** -0.5, 0.09375, ((1, 4),))
    output_basis = normal_values(splits[8], (LIN, D, RANK), D ** -0.5, 0.09375, ((1, 4),))
    queries = normal_values(splits[9], (NL, SK, QUERIES), 0.03, 0.19921875, ((1, 4), (2, 8)))
    return {"token_ids": token_ids, "lengths": lengths, "embed_grads": embed_grads, "vocab_basis": vocab_basis, "embed_basis": embed_basis, "layer_inputs": layer_inputs, "layer_grads": layer_grads, "input_basis": input_basis, "output_basis": output_basis, "queries": queries}


damping = 0.01
epsilon = 1e-6
highest = lax.Precision.HIGHEST


def solve_columns(gram_mat, right_side, count):
    solution = jnp.zeros_like(right_side)
    residual = right_side
    direction = right_side
    norm_now = jnp.sum(residual * residual, axis=0)
    for iteration in range(ITERS):
        images = jnp.dot(gram_mat, direction, precision=highest) / count + damping * direction
        step_size = norm_now / (jnp.sum(direction * images, axis=0) + epsilon)
        solution = solution + step_size * direction
        residual = residual - step_size * images
        norm_next = jnp.sum(residual * residual, axis=0)
        direction = residual + (norm_next / (norm_now + epsilon)) * direction
        norm_now = norm_next
    return solution


def reference(token_ids, lengths, embed_grads, vocab_basis, embed_basis, layer_inputs, layer_grads, input_basis, output_basis, queries):
    pairs = [(jnp.dot(embed_grads, embed_basis, preferred_element_type=jnp.float32),
              vocab_basis[token_ids].astype(jnp.float32))]
    for layer_idx in range(LIN):
        pairs.append((jnp.dot(layer_grads[layer_idx], output_basis[layer_idx], preferred_element_type=jnp.float32),
                      jnp.dot(layer_inputs[layer_idx], input_basis[layer_idx], preferred_element_type=jnp.float32)))
    inverse_len = 1.0 / lengths.astype(jnp.float32)
    position = jnp.arange(SLOT, dtype=jnp.int32)
    weights = jnp.where(position[None, :] < lengths[:, None], inverse_len[:, None], jnp.float32(0.0))
    scores = jnp.zeros((EXAMPLES, QUERIES), jnp.float32)
    for layer_idx in range(NL):
        grads_proj, inputs_proj = pairs[layer_idx]
        weighted = grads_proj.reshape(EXAMPLES, SLOT, RANK) * weights[:, :, None]
        sketches = jnp.einsum('sti,stj->sij', weighted, inputs_proj.reshape(EXAMPLES, SLOT, RANK),
                              precision=highest).reshape(EXAMPLES, RANK * RANK)
        gram_mat = jnp.dot(sketches.T, sketches, precision=highest)
        solution = solve_columns(gram_mat, queries[layer_idx].astype(jnp.float32), EXAMPLES)
        scores = scores + jnp.dot(sketches, solution, precision=highest)
    return scores
```

```python
import functools

import jax
import jax.numpy as jnp
from jax import lax
from jax.experimental import pallas as pl
from jax.experimental.pallas import tpu as pltpu
from jax.sharding import PartitionSpec as P

ITERS = 2
LANES = 128
GROUP = 8

damping = 0.01
epsilon = 1e-06
highest = lax.Precision.HIGHEST


def solve_columns(right_side, apply_operator, column_norm, column_curve):
    solution = jnp.zeros_like(right_side)
    residual = right_side
    direction = right_side
    norm_now = column_norm(residual)
    for iteration in range(ITERS):
        images = apply_operator(direction)
        step_size = norm_now / (column_curve(direction, images) + epsilon)
        solution = solution + step_size[:, None, :] * direction
        residual = residual - step_size[:, None, :] * images
        norm_next = column_norm(residual)
        direction = residual + (norm_next / (norm_now + epsilon))[:, None, :] * direction
        norm_now = norm_next
    return solution


def general_device(
    token_ids,
    lengths,
    embed_grads,
    vocab_basis,
    embed_basis,
    layer_inputs,
    layer_grads,
    input_basis,
    output_basis,
    queries,
):
    vocab_rows = vocab_basis.shape[0]
    basis_rank = embed_basis.shape[1]
    layer_count = layer_inputs.shape[0] + 1
    seq_count = lengths.shape[0]
    token_count = token_ids.shape[0]
    slot_len = token_count // seq_count
    sketch_len = basis_rank * basis_rank
    mp_index = lax.axis_index("mp")
    local_ids = token_ids - mp_index * vocab_rows
    inside = (local_ids >= 0) & (local_ids < vocab_rows)
    looked = jnp.take(vocab_basis, jnp.clip(local_ids, 0, vocab_rows - 1), axis=0)
    pieces = [
        jnp.dot(embed_grads, embed_basis, preferred_element_type=jnp.float32),
        jnp.where(inside[:, None], looked.astype(jnp.float32), 0.0),
    ]
    for layer in range(layer_count - 1):
        pieces.append(jnp.dot(layer_grads[layer], output_basis[layer], preferred_element_type=jnp.float32))
        pieces.append(jnp.dot(layer_inputs[layer], input_basis[layer], preferred_element_type=jnp.float32))
    projected = jnp.concatenate(pieces, axis=1)
    inverse_len = 1.0 / lengths.astype(jnp.float32)
    summed = lax.psum(projected, "mp")
    layout = summed.reshape(seq_count, slot_len, layer_count, 2, basis_rank)
    position = jnp.arange(slot_len, dtype=jnp.int32)
    weights = jnp.where(position[None, :] < lengths[:, None], inverse_len[:, None], 0.0)
    weighted = layout[:, :, :, 0, :] * weights[:, :, None, None]
    sketches = jnp.einsum(
        "stli,stlj->lsij", weighted, layout[:, :, :, 1, :], precision=highest
    ).reshape(layer_count, seq_count, sketch_len)
    examples = seq_count * lax.axis_size("dp")
    targets = lax.all_gather(queries, "dp", axis=2, tiled=True)
    everyone = lax.all_gather(sketches, "dp", axis=1, tiled=True)
    columns = lax.all_to_all(targets, "mp", split_axis=2, concat_axis=1, tiled=True)

    def apply_sketch(direction):
        inner_sums = jnp.einsum("lek,lkq->leq", everyone, direction, precision=highest)
        back_proj = jnp.einsum("lek,leq->lkq", everyone, inner_sums, precision=highest)
        return back_proj / examples + damping * direction

    def local_norm(residual):
        return jnp.sum(residual * residual, axis=1)

    def local_curve(direction, images):
        return jnp.sum(direction * images, axis=1)

    solution = solve_columns(columns.astype(jnp.float32), apply_sketch, local_norm, local_curve)
    partial_value = jnp.einsum("lek,lkq->eq", sketches, solution, precision=highest)
    return lax.all_gather(partial_value, "mp", axis=1, tiled=True)


def contract_last(left, right):
    return lax.dot_general(left, right, (((1,), (1,)), ((), ())), preferred_element_type=jnp.float32)


def project_kernel(
    vocab_rows,
    rank,
    slot_len,
    per_member,
    ids_ref,
    len_ref,
    me_ref,
    row_ids_ref,
    table_ref,
    grad0_ref,
    grad1_ref,
    input1_ref,
    basis0_ref,
    basis1_ref,
    basis2_ref,
    out_ref,
    weight_ref,
):
    step = pl.program_id(0)
    me = me_ref[0]
    member = me ^ step

    @pl.when(step == 0)
    def _():
        weight_ref[...] = jnp.zeros_like(weight_ref)
        for place, basis in enumerate((basis0_ref, basis1_ref, basis2_ref)):
            weight_ref[place, place * rank : (place + 1) * rank, :] = basis[...]

    tiles = (vocab_rows + LANES - 1) // LANES
    lane = lax.broadcasted_iota(jnp.int32, (rank, LANES), 1)
    offset = me * vocab_rows
    for s in range(per_member):
        seq = member * per_member + s

        def body(group, found, seq=seq):
            for j in range(GROUP):
                t = group * GROUP + j
                local = ids_ref[seq * slot_len + t] - offset
                tile = jnp.clip(local >> 7, 0, tiles - 1)
                block = table_ref[:, pl.ds(pl.multiple_of(tile * LANES, LANES), LANES)]
                turned = pltpu.roll(block.astype(jnp.float32), (t - local) & (LANES - 1), 1)
                found = jnp.where(lane == t, turned, found)
            return found

        groups = (len_ref[seq] + (GROUP - 1)) // GROUP
        found = lax.fori_loop(0, groups, body, jnp.zeros((rank, LANES), jnp.float32))
        local = row_ids_ref[pl.ds(seq, 1), :] - offset
        inside = (local >= 0) & (local < vocab_rows)
        found = jnp.where(inside, found, 0.0)
        rows = slice(s * slot_len, (s + 1) * slot_len)
        total = contract_last(grad0_ref[rows, :], weight_ref[0])
        total += contract_last(grad1_ref[rows, :], weight_ref[1])
        total += contract_last(input1_ref[rows, :], weight_ref[2])
        spread = jnp.concatenate([jnp.zeros((3 * rank, LANES), jnp.float32), found], axis=0)
        out_ref[0, rows, :] = total + spread.T


def sketch_kernel(rank, slot_len, per_member, len_ref, me_ref, *refs):
    parts, out_ref, full_ref = refs[:-2], refs[-2], refs[-1]
    me = me_ref[0]
    lane = lax.broadcasted_iota(jnp.int32, (8, LANES), 1)
    for s in range(per_member):
        rows = slice(s * slot_len, (s + 1) * slot_len)
        total = parts[0][rows, :]
        for part in parts[1:]:
            total = total + part[rows, :]
        live = len_ref[me * per_member + s]
        position = lax.broadcasted_iota(jnp.int32, (slot_len, LANES), 0)
        share = 1.0 / jnp.full((slot_len, LANES), live, jnp.int32).astype(jnp.float32)
        weighted = total * jnp.where(position < live, share, 0.0)
        full_ref[s] = lax.dot_general(
            weighted, total, (((0,), (0,)), ((), ())), precision=highest, preferred_element_type=jnp.float32
        )
        for layer in range(2):
            source = 3 - layer
            unit = jnp.zeros((8, LANES), jnp.float32)
            for c in range(4):
                piece = full_ref[s, pl.ds(layer * rank + c, 8, stride=4), :]
                turned = pltpu.roll(piece, ((c - source) * rank) % LANES, 1)
                unit = jnp.where((lane >= c * rank) & (lane < (c + 1) * rank), turned, unit)
            out_ref[pl.ds((s * 2 + layer) * 8, 8), :] = unit


def swap_blocks(value, axis, width, index, count):
    size = value.shape[axis]
    place = lax.broadcasted_iota(jnp.int32, value.shape, axis)
    bit = 1
    while bit < count:
        shift = bit * width
        up = pltpu.roll(value, shift, axis)
        down = pltpu.roll(value, size - shift, axis)
        other = jnp.where((place // shift) % 2 == 1, up, down)
        value = jnp.where((index // bit) % 2 == 1, other, value)
        bit *= 2
    return value


def solve_kernel(mp, zs, per_member, examples, me_ref, dp_ref, mine_ref, other_ref, qmine_ref, qother_ref, norm_ref, out_ref):
    me = me_ref[0]
    half = mp * zs * per_member
    columns = qmine_ref.shape[1] * qmine_ref.shape[3]
    chunk = qmine_ref.shape[4]
    scores = None
    for layer in range(2):
        square = jnp.zeros((4 * half, 4 * half), jnp.float32)
        mixed = [jnp.zeros((4 * half, columns), jnp.float32) for _ in range(2)]
        for k in range(mp):
            first = (me ^ k) * (chunk // LANES)
            wide = []
            for j in range(chunk // LANES):
                start = layer * 8 + first + j
                wide.append(
                    jnp.concatenate(
                        [ref[pl.ds(start, half, stride=16), :] for ref in (mine_ref, other_ref)], axis=0
                    )
                )
            value = jnp.concatenate(wide, axis=1)
            high = value.astype(jnp.bfloat16)
            low = (value - high.astype(jnp.float32)).astype(jnp.bfloat16)
            both = jnp.concatenate([high, low], axis=0)
            square += contract_last(both, both)
            for side, ref in enumerate((qmine_ref, qother_ref)):
                mixed[side] += contract_last(both, ref[k, :, layer].reshape(columns, chunk))
        n = 2 * half
        gram = square[:n, :n] + square[:n, n:] + square[n:, :n] + square[n:, n:]
        u = jnp.concatenate([m[:n] + m[n:] for m in mixed], axis=1)
        ku = jnp.dot(gram, u, precision=highest, preferred_element_type=jnp.float32)
        qq = norm_ref[layer]
        uu = jnp.sum(u * u, axis=0, keepdims=True)
        uku = jnp.sum(u * ku, axis=0, keepdims=True)
        step0 = qq / (uu / examples + damping * qq + epsilon)
        alpha = 1.0 - damping * step0
        beta = -step0 / examples
        rr = jnp.maximum(alpha * alpha * qq + 2.0 * alpha * beta * uu + beta * beta * uku, 0.0)
        a = alpha + rr / (qq + epsilon)
        sd = a * u + beta * ku
        dd = jnp.maximum(a * a * qq + 2.0 * a * beta * uu + beta * beta * uku, 0.0)
        step1 = rr / (jnp.sum(sd * sd, axis=0, keepdims=True) / examples + damping * dd + epsilon)
        value = step0 * u + step1 * sd
        scores = value if scores is None else scores + value
    own = jnp.concatenate(
        [scores[k * zs * per_member : k * zs * per_member + per_member] for k in range(mp)], axis=0
    )
    own = swap_blocks(own, 0, per_member, me, mp)
    width = columns // zs
    own = jnp.concatenate(
        [own[:, (c * zs + z) * width : (c * zs + z + 1) * width] for z in range(zs) for c in range(2)], axis=1
    )
    out_ref[...] = swap_blocks(own, 1, width, dp_ref[0], 2 * zs)


def exchange(value, axis, count, unit=1):
    size = lax.axis_size(axis)
    return [value] + [
        lax.ppermute(value, axis, [(i, i ^ (k * unit)) for i in range(size)]) for k in range(1, count)
    ]


def fast_device(
    token_ids,
    lengths,
    embed_grads,
    vocab_basis,
    embed_basis,
    layer_inputs,
    layer_grads,
    input_basis,
    output_basis,
    queries,
):
    vocab_rows, rank = vocab_basis.shape
    seq_count = lengths.shape[0]
    token_count, features = embed_grads.shape
    slot_len = token_count // seq_count
    mp, dp = lax.axis_size("mp"), lax.axis_size("dp")
    zs = dp // 2
    per_member = seq_count // mp
    examples = seq_count * dp
    me = lax.axis_index("mp").astype(jnp.int32)[None]
    mydp = lax.axis_index("dp").astype(jnp.int32)[None]
    smem = pl.BlockSpec(memory_space=pltpu.SMEM)

    qt = queries.transpose(0, 2, 1)
    qz = jnp.stack(exchange(qt, "dp", zs, 2))
    qall = jnp.stack(exchange(qz, "mp", mp))
    qcore = exchange(qall, "dp", 2)[1]

    def norms(value):
        return jnp.sum(jnp.square(value.astype(jnp.float32)), axis=(0, 4)).transpose(1, 0, 2).reshape(2, 1, -1)

    norm = jnp.concatenate([norms(qall), norms(qcore)], axis=2)

    block = per_member * slot_len
    row_block = lambda r, ids, lens, me: (me[0] ^ r, 0)
    fixed = lambda r, ids, lens, me: (0, 0)
    padded = (vocab_rows + LANES - 1) // LANES * LANES
    sent = pl.pallas_call(
        functools.partial(project_kernel, vocab_rows, rank, slot_len, per_member),
        out_shape=jax.ShapeDtypeStruct((mp, block, LANES), jnp.float32),
        grid_spec=pltpu.PrefetchScalarGridSpec(
            num_scalar_prefetch=3,
            grid=(mp,),
            in_specs=[
                pl.BlockSpec((seq_count, slot_len), fixed),
                pl.BlockSpec((rank, padded), fixed),
                pl.BlockSpec((block, features), row_block),
                pl.BlockSpec((block, features), row_block),
                pl.BlockSpec((block, features), row_block),
                pl.BlockSpec((rank, features), fixed),
                pl.BlockSpec((rank, features), fixed),
                pl.BlockSpec((rank, features), fixed),
            ],
            out_specs=pl.BlockSpec((1, block, LANES), lambda r, ids, lens, me: (r, 0, 0)),
            scratch_shapes=[pltpu.VMEM((3, LANES, features), jnp.bfloat16)],
        ),
        name="project",
    )(
        token_ids,
        lengths,
        me,
        token_ids.reshape(seq_count, slot_len),
        vocab_basis.T,
        embed_grads,
        layer_grads[0],
        layer_inputs[0],
        embed_basis.T,
        output_basis[0].T,
        input_basis[0].T,
    )
    parts = [sent[0]] + [
        lax.ppermute(sent[k], "mp", [(i, i ^ k) for i in range(mp)]) for k in range(1, mp)
    ]
    rows = per_member * 2 * 8
    whole = lambda n: [pl.BlockSpec(memory_space=pltpu.VMEM)] * n
    units = pl.pallas_call(
        functools.partial(sketch_kernel, rank, slot_len, per_member),
        out_shape=jax.ShapeDtypeStruct((rows, LANES), jnp.float32),
        in_specs=[smem, smem] + whole(mp),
        out_specs=pl.BlockSpec(memory_space=pltpu.VMEM),
        scratch_shapes=[pltpu.VMEM((per_member, LANES, LANES), jnp.float32)],
        name="sketch",
    )(lengths, me, *parts)
    along_z = jnp.concatenate(exchange(units, "dp", zs, 2))
    mine = jnp.concatenate(exchange(along_z, "mp", mp))
    other = exchange(mine, "dp", 2)[1]
    return pl.pallas_call(
        functools.partial(solve_kernel, mp, zs, per_member, examples),
        out_shape=jax.ShapeDtypeStruct((seq_count, queries.shape[2] * dp), jnp.float32),
        in_specs=[smem, smem] + whole(5),
        out_specs=pl.BlockSpec(memory_space=pltpu.VMEM),
        name="solve",
    )(me, mydp, mine, other, qall, qcore, norm)


def power_of_two(n):
    return n & (n - 1) == 0


def solution(mesh):
    placed = (
        P("dp"),
        P("dp"),
        P("dp", "mp"),
        P("mp", None),
        P("mp", None),
        P(None, "dp", "mp"),
        P(None, "dp", "mp"),
        P(None, "mp", None),
        P(None, "mp", None),
        P(None, "mp", "dp"),
    )

    def per_device(*args):
        mp, dp = mesh.shape["mp"], mesh.shape["dp"]
        token_ids, lengths, layer_inputs, queries = args[0], args[1], args[5], args[9]
        seq_count, rank = lengths.shape[0], args[3].shape[1]
        fits = (
            layer_inputs.shape[0] == 1
            and token_ids.shape[0] == seq_count * LANES
            and rank * 4 == LANES
            and seq_count % 8 == 0
            and seq_count % mp == 0
            and power_of_two(mp)
            and power_of_two(dp)
            and dp % 2 == 0
            and queries.shape[1] % LANES == 0
            and queries.shape[2] % 16 == 0
            and queries.shape[2] * dp // 2 == LANES
        )
        return (fast_device if fits else general_device)(*args)

    return jax.shard_map(per_device, mesh=mesh, in_specs=placed, out_specs=P("dp", None), check_vma=False)
```

```python
import functools

import jax
import jax.numpy as jnp
from jax import lax
from jax.experimental import pallas as pl
from jax.experimental.pallas import tpu as pltpu
from jax.sharding import PartitionSpec as P


ITERS = 2
LANES = 128

damping = 0.01
epsilon = 1e-06
highest = lax.Precision.HIGHEST


def solve_columns(right_side, apply_operator, column_norm, column_curve):
    solution = jnp.zeros_like(right_side)
    residual = right_side
    direction = right_side
    norm_now = column_norm(residual)
    for _ in range(ITERS):
        images = apply_operator(direction)
        step_size = norm_now / (column_curve(direction, images) + epsilon)
        solution = solution + step_size[:, None, :] * direction
        residual = residual - step_size[:, None, :] * images
        norm_next = column_norm(residual)
        direction = residual + (norm_next / (norm_now + epsilon))[:, None, :] * direction
        norm_now = norm_next
    return solution


def general_device(
    token_ids,
    lengths,
    embed_grads,
    vocab_basis,
    embed_basis,
    layer_inputs,
    layer_grads,
    input_basis,
    output_basis,
    queries,
):
    vocab_rows = vocab_basis.shape[0]
    basis_rank = embed_basis.shape[1]
    layer_count = layer_inputs.shape[0] + 1
    seq_count = lengths.shape[0]
    token_count = token_ids.shape[0]
    slot_len = token_count // seq_count
    sketch_len = basis_rank * basis_rank
    mp_index = lax.axis_index("mp")
    local_ids = token_ids - mp_index * vocab_rows
    inside = (local_ids >= 0) & (local_ids < vocab_rows)
    looked = jnp.take(vocab_basis, jnp.clip(local_ids, 0, vocab_rows - 1), axis=0)
    pieces = [
        jnp.dot(embed_grads, embed_basis, preferred_element_type=jnp.float32),
        jnp.where(inside[:, None], looked.astype(jnp.float32), 0.0),
    ]
    for layer in range(layer_count - 1):
        pieces.append(jnp.dot(layer_grads[layer], output_basis[layer], preferred_element_type=jnp.float32))
        pieces.append(jnp.dot(layer_inputs[layer], input_basis[layer], preferred_element_type=jnp.float32))
    projected = jnp.concatenate(pieces, axis=1)
    inverse_len = 1.0 / lengths.astype(jnp.float32)
    summed = lax.psum(projected, "mp")
    layout = summed.reshape(seq_count, slot_len, layer_count, 2, basis_rank)
    position = jnp.arange(slot_len, dtype=jnp.int32)
    weights = jnp.where(position[None, :] < lengths[:, None], inverse_len[:, None], 0.0)
    weighted = layout[:, :, :, 0, :] * weights[:, :, None, None]
    sketches = jnp.einsum(
        "stli,stlj->lsij", weighted, layout[:, :, :, 1, :], precision=highest
    ).reshape(layer_count, seq_count, sketch_len)
    examples = seq_count * lax.axis_size("dp")
    targets = lax.all_gather(queries, "dp", axis=2, tiled=True)
    everyone = lax.all_gather(sketches, "dp", axis=1, tiled=True)
    columns = lax.all_to_all(targets, "mp", split_axis=2, concat_axis=1, tiled=True)

    def apply_sketch(direction):
        inner_sums = jnp.einsum("lek,lkq->leq", everyone, direction, precision=highest)
        back_proj = jnp.einsum("lek,leq->lkq", everyone, inner_sums, precision=highest)
        return back_proj / examples + damping * direction

    def local_norm(residual):
        return jnp.sum(residual * residual, axis=1)

    def local_curve(direction, images):
        return jnp.sum(direction * images, axis=1)

    solution = solve_columns(columns.astype(jnp.float32), apply_sketch, local_norm, local_curve)
    partial_value = jnp.einsum("lek,lkq->eq", sketches, solution, precision=highest)
    return lax.all_gather(partial_value, "mp", axis=1, tiled=True)


def contract_last(left, right):
    return lax.dot_general(left, right, (((1,), (1,)), ((), ())), preferred_element_type=jnp.float32)


def project_kernel(
    vocab_rows,
    rank,
    slot_len,
    per_member,
    ids_any,
    table_any,
    grad0_any,
    grad1_any,
    input1_any,
    basis0_any,
    basis1_any,
    basis2_any,
    *refs,
):
    out_refs = refs[:-8]
    ids_ref, table_ref, wide_ref, weight_ref, place_ref, scalar_ref, small_sem, wide_sem = refs[-8:]
    members = len(out_refs)
    me = lax.axis_index("mp").astype(jnp.int32)
    offset = me * vocab_rows
    main = vocab_rows // LANES
    block = per_member * slot_len

    def rows_of(r):
        return pl.ds(pl.multiple_of((me ^ r) * block, block), block)

    def wide_copy(k, r):
        source = (grad0_any, grad1_any, input1_any)[k]
        return pltpu.make_async_copy(source.at[rows_of(r), :], wide_ref.at[k, rows_of(r), :], wide_sem.at[k, r])

    ids_copy = pltpu.make_async_copy(ids_any, ids_ref, small_sem.at[0])
    table_copy = pltpu.make_async_copy(table_any, table_ref, small_sem.at[1])
    basis_copies = [
        pltpu.make_async_copy(basis, weight_ref.at[k, pl.ds(k * rank, rank), :], small_sem.at[2 + k])
        for k, basis in enumerate((basis0_any, basis1_any, basis2_any))
    ]
    ids_copy.start()
    table_copy.start()
    for copy in basis_copies:
        copy.start()
    for r in range(members):
        for k in range(3):
            wide_copy(k, r).start()
    for k in range(3):
        if k:
            weight_ref[k, : k * rank, :] = jnp.zeros((k * rank, weight_ref.shape[2]), jnp.bfloat16)
        weight_ref[k, (k + 1) * rank :, :] = jnp.zeros((LANES - (k + 1) * rank, weight_ref.shape[2]), jnp.bfloat16)
    ids_copy.wait()
    local = ids_ref[...] - offset
    position = lax.broadcasted_iota(jnp.int32, local.shape, 1)
    place_ref[0] = jnp.clip(local >> 7, 0, main - 1) * LANES
    place_ref[1] = (position - local) & (LANES - 1)
    scalar_copy = pltpu.make_async_copy(place_ref, scalar_ref, small_sem.at[0])
    scalar_copy.start()
    scalar_copy.wait()
    table_copy.wait()
    for copy in basis_copies:
        copy.wait()

    lane = lax.broadcasted_iota(jnp.int32, (rank, LANES), 1)
    tail = vocab_rows - main * LANES

    def step(r, _):
        member = me ^ r
        values = []
        for k in range(3):
            wide_copy(k, r).wait()
        for s in range(per_member):
            seq = member * per_member + s
            found = jnp.zeros((rank, LANES), jnp.float32)
            for t in range(slot_len):
                start = pl.multiple_of(scalar_ref[0, seq, t], LANES)
                block = table_ref[:, pl.ds(start, LANES)].astype(jnp.float32)
                found = jnp.where(lane == t, pltpu.roll(block, scalar_ref[1, seq, t], 1), found)
            mine = ids_ref[pl.ds(seq, 1), :] - offset
            found = jnp.where((mine >= 0) & (mine < main * LANES), found, 0.0)
            if tail:
                sub = lax.broadcasted_iota(jnp.int32, (tail, LANES), 0)
                pick = jnp.where(mine - main * LANES == sub, 1.0, 0.0).astype(jnp.bfloat16)
                found += jnp.dot(table_ref[:, main * LANES :], pick, preferred_element_type=jnp.float32)
            rows = pl.ds(pl.multiple_of(seq * slot_len, slot_len), slot_len)
            total = contract_last(wide_ref[0, rows, :], weight_ref[0])
            total += contract_last(wide_ref[1, rows, :], weight_ref[1])
            total += contract_last(wide_ref[2, rows, :], weight_ref[2])
            spread = jnp.concatenate([jnp.zeros((3 * rank, LANES), jnp.float32), found], axis=0)
            values.append(total + spread.T)
        for place, out_ref in enumerate(out_refs):

            @pl.when(r == place)
            def _():
                for s in range(per_member):
                    out_ref[s * slot_len : (s + 1) * slot_len, :] = values[s]

        return 0

    lax.fori_loop(0, members, step, 0)


def sketch_kernel(rank, slot_len, per_member, len_ref, *refs):
    parts, out_ref, full_ref = refs[:-2], refs[-2], refs[-1]
    me = lax.axis_index("mp").astype(jnp.int32)
    lane = lax.broadcasted_iota(jnp.int32, (8, LANES), 1)
    for s in range(per_member):
        rows = slice(s * slot_len, (s + 1) * slot_len)
        total = parts[0][rows, :]
        for part in parts[1:]:
            total = total + part[rows, :]
        live = len_ref[me * per_member + s]
        position = lax.broadcasted_iota(jnp.int32, (slot_len, LANES), 0)
        share = 1.0 / jnp.full((slot_len, LANES), live, jnp.int32).astype(jnp.float32)
        weighted = total * jnp.where(position < live, share, 0.0)
        full_ref[s] = lax.dot_general(
            weighted, total, (((0,), (0,)), ((), ())), precision=highest, preferred_element_type=jnp.float32
        )
        for layer in range(2):
            source = 3 - layer
            unit = jnp.zeros((8, LANES), jnp.float32)
            for c in range(4):
                piece = full_ref[s, pl.ds(layer * rank + c, 8, stride=4), :]
                turned = pltpu.roll(piece, ((c - source) * rank) % LANES, 1)
                unit = jnp.where((lane >= c * rank) & (lane < (c + 1) * rank), turned, unit)
            out_ref[pl.ds((s * 2 + layer) * 8, 8), :] = unit


def swap_blocks(value, axis, width, index, count):
    size = value.shape[axis]
    place = lax.broadcasted_iota(jnp.int32, value.shape, axis)
    bit = 1
    while bit < count:
        shift = bit * width
        up = pltpu.roll(value, shift, axis)
        down = pltpu.roll(value, size - shift, axis)
        other = jnp.where((place // shift) % 2 == 1, up, down)
        value = jnp.where((index // bit) % 2 == 1, other, value)
        bit *= 2
    return value


def solve_kernel(mp, zs, per_member, examples, mine_ref, other_ref, qmine_ref, qother_ref, out_ref):
    me = lax.axis_index("mp").astype(jnp.int32)
    mydp = lax.axis_index("dp").astype(jnp.int32)
    half = mp * zs * per_member
    columns = qmine_ref.shape[1] * qmine_ref.shape[3]
    chunk = qmine_ref.shape[4]
    scores = None
    for layer in range(2):
        square = jnp.zeros((4 * half, 4 * half), jnp.float32)
        mixed = [jnp.zeros((4 * half, columns), jnp.float32) for _ in range(2)]
        norms = [jnp.zeros((columns, LANES), jnp.float32) for _ in range(2)]
        for k in range(mp):
            first = (me ^ k) * (chunk // LANES)
            wide = []
            for j in range(chunk // LANES):
                start = layer * 8 + first + j
                wide.append(
                    jnp.concatenate(
                        [ref[pl.ds(start, half, stride=16), :] for ref in (mine_ref, other_ref)], axis=0
                    )
                )
            value = jnp.concatenate(wide, axis=1)
            high = value.astype(jnp.bfloat16)
            low = (value - high.astype(jnp.float32)).astype(jnp.bfloat16)
            both = jnp.concatenate([high, low], axis=0)
            square += contract_last(both, both)
            for side, ref in enumerate((qmine_ref, qother_ref)):
                query = ref[k, :, layer].reshape(columns, chunk)
                mixed[side] += contract_last(both, query)
                wide_query = query.astype(jnp.float32)
                squared = wide_query * wide_query
                for j in range(chunk // LANES):
                    norms[side] += squared[:, j * LANES : (j + 1) * LANES]
        n = 2 * half
        gram = square[:n, :n] + square[:n, n:] + square[n:, :n] + square[n:, n:]
        u = jnp.concatenate([m[:n] + m[n:] for m in mixed], axis=1)
        ku = jnp.dot(gram, u, precision=highest, preferred_element_type=jnp.float32)
        qq = lax.dot_general(
            jnp.ones((8, LANES), jnp.float32),
            jnp.concatenate(norms, axis=0),
            (((1,), (1,)), ((), ())),
            precision=highest,
            preferred_element_type=jnp.float32,
        )[:1]
        uu = jnp.sum(u * u, axis=0, keepdims=True)
        uku = jnp.sum(u * ku, axis=0, keepdims=True)
        step0 = qq / (uu / examples + damping * qq + epsilon)
        alpha = 1.0 - damping * step0
        beta = -step0 / examples
        rr = jnp.maximum(alpha * alpha * qq + 2.0 * alpha * beta * uu + beta * beta * uku, 0.0)
        a = alpha + rr / (qq + epsilon)
        sd = a * u + beta * ku
        dd = jnp.maximum(a * a * qq + 2.0 * a * beta * uu + beta * beta * uku, 0.0)
        step1 = rr / (jnp.sum(sd * sd, axis=0, keepdims=True) / examples + damping * dd + epsilon)
        value = step0 * u + step1 * sd
        scores = value if scores is None else scores + value
    own = jnp.concatenate(
        [scores[k * zs * per_member : k * zs * per_member + per_member] for k in range(mp)], axis=0
    )
    own = swap_blocks(own, 0, per_member, me, mp)
    width = columns // zs
    own = jnp.concatenate(
        [own[:, (c * zs + z) * width : (c * zs + z + 1) * width] for z in range(zs) for c in range(2)], axis=1
    )
    out_ref[...] = swap_blocks(own, 1, width, mydp, 2 * zs)


def exchange(value, axis, count, unit=1):
    size = lax.axis_size(axis)
    return [value] + [
        lax.ppermute(value, axis, [(i, i ^ (k * unit)) for i in range(size)]) for k in range(1, count)
    ]


def fast_device(
    token_ids,
    lengths,
    embed_grads,
    vocab_basis,
    embed_basis,
    layer_inputs,
    layer_grads,
    input_basis,
    output_basis,
    queries,
):
    vocab_rows, rank = vocab_basis.shape
    seq_count = lengths.shape[0]
    token_count, features = embed_grads.shape
    slot_len = token_count // seq_count
    mp, dp = lax.axis_size("mp"), lax.axis_size("dp")
    zs = dp // 2
    per_member = seq_count // mp
    examples = seq_count * dp
    placed = lambda space, *values: [pltpu.with_memory_space_constraint(v, space) for v in values]
    whole = lambda n: [pl.BlockSpec(memory_space=pltpu.VMEM)] * n
    limit = pltpu.CompilerParams(vmem_limit_bytes=16 * 2**20)

    block = per_member * slot_len
    sent = pl.pallas_call(
        functools.partial(project_kernel, vocab_rows, rank, slot_len, per_member),
        out_shape=[pltpu.VMEM((block, LANES), jnp.float32)] * mp,
        in_specs=[pl.BlockSpec(memory_space=pl.ANY)] * 8,
        out_specs=whole(mp),
        scratch_shapes=[
            pltpu.VMEM((seq_count, slot_len), jnp.int32),
            pltpu.VMEM((rank, vocab_rows), jnp.bfloat16),
            pltpu.VMEM((3, token_count, features), jnp.bfloat16),
            pltpu.VMEM((3, LANES, features), jnp.bfloat16),
            pltpu.VMEM((2, seq_count, slot_len), jnp.int32),
            pltpu.SMEM((2, seq_count, slot_len), jnp.int32),
            pltpu.SemaphoreType.DMA((5,)),
            pltpu.SemaphoreType.DMA((3, mp)),
        ],
        compiler_params=limit,
        name="project",
    )(
        *placed(
            pltpu.HBM,
            token_ids.reshape(seq_count, slot_len),
            vocab_basis.T,
            embed_grads,
            layer_grads[0],
            layer_inputs[0],
            embed_basis.T,
            output_basis[0].T,
            input_basis[0].T,
        )
    )
    parts = [sent[0]]
    for k in range(1, mp):
        parts.append(lax.ppermute(sent[k], "mp", [(i, i ^ k) for i in range(mp)]))

    qt = queries.transpose(0, 2, 1)
    qz = jnp.stack(exchange(qt, "dp", zs, 2))
    qall = jnp.stack(exchange(qz, "mp", mp))
    qcore = exchange(qall, "dp", 2)[1]
    rows = per_member * 2 * 8
    units = pl.pallas_call(
        functools.partial(sketch_kernel, rank, slot_len, per_member),
        out_shape=pltpu.VMEM((rows, LANES), jnp.float32),
        in_specs=[pl.BlockSpec(memory_space=pltpu.SMEM)] + whole(mp),
        out_specs=whole(1)[0],
        scratch_shapes=[pltpu.VMEM((per_member, LANES, LANES), jnp.float32)],
        compiler_params=limit,
        name="sketch",
    )(lengths, *placed(pltpu.VMEM, *parts))
    along_z = jnp.concatenate(exchange(units, "dp", zs, 2))
    mine = jnp.concatenate(exchange(along_z, "mp", mp))
    other = exchange(mine, "dp", 2)[1]
    return pl.pallas_call(
        functools.partial(solve_kernel, mp, zs, per_member, examples),
        out_shape=jax.ShapeDtypeStruct((seq_count, queries.shape[2] * dp), jnp.float32),
        in_specs=whole(4),
        out_specs=whole(1)[0],
        compiler_params=limit,
        name="solve",
    )(*placed(pltpu.VMEM, mine, other, qall, qcore))


def power_of_two(n):
    return n & (n - 1) == 0


def solution(mesh):
    placed = (
        P("dp"),
        P("dp"),
        P("dp", "mp"),
        P("mp", None),
        P("mp", None),
        P(None, "dp", "mp"),
        P(None, "dp", "mp"),
        P(None, "mp", None),
        P(None, "mp", None),
        P(None, "mp", "dp"),
    )

    def per_device(*args):
        mp, dp = mesh.shape["mp"], mesh.shape["dp"]
        token_ids, lengths, layer_inputs, queries = args[0], args[1], args[5], args[9]
        seq_count, rank = lengths.shape[0], args[3].shape[1]
        fits = (
            layer_inputs.shape[0] == 1
            and token_ids.shape[0] == seq_count * LANES
            and rank * 4 == LANES
            and seq_count % 8 == 0
            and seq_count % mp == 0
            and power_of_two(mp)
            and power_of_two(dp)
            and dp % 2 == 0
            and queries.shape[1] % LANES == 0
            and queries.shape[2] % 16 == 0
            and queries.shape[2] * dp // 2 == LANES
        )
        if not fits:
            return general_device(*args)
        return fast_device(*args)

    return jax.shard_map(per_device, mesh=mesh, in_specs=placed, out_specs=P("dp", None), check_vma=False)
```

```python
import functools

import jax
import jax.numpy as jnp
from jax import lax
from jax.experimental import pallas as pl
from jax.experimental.pallas import tpu as pltpu
from jax.sharding import PartitionSpec as P


ITERS = 2
LANES = 128

damping = 0.01
epsilon = 1e-06
highest = lax.Precision.HIGHEST


def solve_columns(right_side, apply_operator, column_norm, column_curve):
    solution = jnp.zeros_like(right_side)
    residual = right_side
    direction = right_side
    norm_now = column_norm(residual)
    for _ in range(ITERS):
        images = apply_operator(direction)
        step_size = norm_now / (column_curve(direction, images) + epsilon)
        solution = solution + step_size[:, None, :] * direction
        residual = residual - step_size[:, None, :] * images
        norm_next = column_norm(residual)
        direction = residual + (norm_next / (norm_now + epsilon))[:, None, :] * direction
        norm_now = norm_next
    return solution


def general_device(
    token_ids,
    lengths,
    embed_grads,
    vocab_basis,
    embed_basis,
    layer_inputs,
    layer_grads,
    input_basis,
    output_basis,
    queries,
):
    vocab_rows = vocab_basis.shape[0]
    basis_rank = embed_basis.shape[1]
    layer_count = layer_inputs.shape[0] + 1
    seq_count = lengths.shape[0]
    token_count = token_ids.shape[0]
    slot_len = token_count // seq_count
    sketch_len = basis_rank * basis_rank
    mp_index = lax.axis_index("mp")
    local_ids = token_ids - mp_index * vocab_rows
    inside = (local_ids >= 0) & (local_ids < vocab_rows)
    looked = jnp.take(vocab_basis, jnp.clip(local_ids, 0, vocab_rows - 1), axis=0)
    pieces = [
        jnp.dot(embed_grads, embed_basis, preferred_element_type=jnp.float32),
        jnp.where(inside[:, None], looked.astype(jnp.float32), 0.0),
    ]
    for layer in range(layer_count - 1):
        pieces.append(jnp.dot(layer_grads[layer], output_basis[layer], preferred_element_type=jnp.float32))
        pieces.append(jnp.dot(layer_inputs[layer], input_basis[layer], preferred_element_type=jnp.float32))
    projected = jnp.concatenate(pieces, axis=1)
    inverse_len = 1.0 / lengths.astype(jnp.float32)
    summed = lax.psum(projected, "mp")
    layout = summed.reshape(seq_count, slot_len, layer_count, 2, basis_rank)
    position = jnp.arange(slot_len, dtype=jnp.int32)
    weights = jnp.where(position[None, :] < lengths[:, None], inverse_len[:, None], 0.0)
    weighted = layout[:, :, :, 0, :] * weights[:, :, None, None]
    sketches = jnp.einsum(
        "stli,stlj->lsij", weighted, layout[:, :, :, 1, :], precision=highest
    ).reshape(layer_count, seq_count, sketch_len)
    examples = seq_count * lax.axis_size("dp")
    targets = lax.all_gather(queries, "dp", axis=2, tiled=True)
    everyone = lax.all_gather(sketches, "dp", axis=1, tiled=True)
    columns = lax.all_to_all(targets, "mp", split_axis=2, concat_axis=1, tiled=True)

    def apply_sketch(direction):
        inner_sums = jnp.einsum("lek,lkq->leq", everyone, direction, precision=highest)
        back_proj = jnp.einsum("lek,leq->lkq", everyone, inner_sums, precision=highest)
        return back_proj / examples + damping * direction

    def local_norm(residual):
        return jnp.sum(residual * residual, axis=1)

    def local_curve(direction, images):
        return jnp.sum(direction * images, axis=1)

    solution = solve_columns(columns.astype(jnp.float32), apply_sketch, local_norm, local_curve)
    partial_value = jnp.einsum("lek,lkq->eq", sketches, solution, precision=highest)
    return lax.all_gather(partial_value, "mp", axis=1, tiled=True)


def contract_last(left, right):
    return lax.dot_general(left, right, (((1,), (1,)), ((), ())), preferred_element_type=jnp.float32)


def project_kernel(
    vocab_rows,
    rank,
    slot_len,
    per_member,
    ids_any,
    table_any,
    grad0_any,
    grad1_any,
    input1_any,
    basis0_any,
    basis1_any,
    basis2_any,
    *refs,
):
    out_refs = refs[:-8]
    ids_ref, table_ref, wide_ref, weight_ref, place_ref, scalar_ref, small_sem, wide_sem = refs[-8:]
    members = len(out_refs)
    me = lax.axis_index("mp").astype(jnp.int32)
    offset = me * vocab_rows
    main = vocab_rows // LANES
    block = per_member * slot_len

    def rows_of(r):
        return pl.ds(pl.multiple_of((me ^ r) * block, block), block)

    def wide_copy(k, r):
        source = (grad0_any, grad1_any, input1_any)[k]
        return pltpu.make_async_copy(source.at[rows_of(r), :], wide_ref.at[k, rows_of(r), :], wide_sem.at[k, r])

    ids_copy = pltpu.make_async_copy(ids_any, ids_ref, small_sem.at[0])
    table_copy = pltpu.make_async_copy(table_any, table_ref, small_sem.at[1])
    basis_copies = [
        pltpu.make_async_copy(basis, weight_ref.at[k, pl.ds(k * rank, rank), :], small_sem.at[2 + k])
        for k, basis in enumerate((basis0_any, basis1_any, basis2_any))
    ]
    ids_copy.start()
    for copy in basis_copies:
        copy.start()
    table_copy.start()
    for k in range(3):
        wide_copy(k, 0).start()
    for k in range(3):
        if k:
            weight_ref[k, : k * rank, :] = jnp.zeros((k * rank, weight_ref.shape[2]), jnp.bfloat16)
        weight_ref[k, (k + 1) * rank :, :] = jnp.zeros((LANES - (k + 1) * rank, weight_ref.shape[2]), jnp.bfloat16)
    ids_copy.wait()
    local = ids_ref[...] - offset
    position = lax.broadcasted_iota(jnp.int32, local.shape, 1)
    place_ref[0] = jnp.clip(local >> 7, 0, main - 1) * LANES
    place_ref[1] = (position - local) & (LANES - 1)
    scalar_copy = pltpu.make_async_copy(place_ref, scalar_ref, small_sem.at[0])
    scalar_copy.start()
    scalar_copy.wait()
    for copy in basis_copies:
        copy.wait()
    table_copy.wait()
    for r in range(1, members):
        for k in range(3):
            wide_copy(k, r).start()

    lane = lax.broadcasted_iota(jnp.int32, (rank, LANES), 1)
    tail = vocab_rows - main * LANES

    def step(r, _):
        member = me ^ r
        values = []
        for k in range(3):
            wide_copy(k, r).wait()
        for s in range(per_member):
            seq = member * per_member + s
            found = jnp.zeros((rank, LANES), jnp.float32)
            for t in range(slot_len):
                start = pl.multiple_of(scalar_ref[0, seq, t], LANES)
                block = table_ref[:, pl.ds(start, LANES)].astype(jnp.float32)
                found = jnp.where(lane == t, pltpu.roll(block, scalar_ref[1, seq, t], 1), found)
            mine = ids_ref[pl.ds(seq, 1), :] - offset
            found = jnp.where((mine >= 0) & (mine < main * LANES), found, 0.0)
            if tail:
                sub = lax.broadcasted_iota(jnp.int32, (tail, LANES), 0)
                pick = jnp.where(mine - main * LANES == sub, 1.0, 0.0).astype(jnp.bfloat16)
                found += jnp.dot(table_ref[:, main * LANES :], pick, preferred_element_type=jnp.float32)
            rows = pl.ds(pl.multiple_of(seq * slot_len, slot_len), slot_len)
            total = contract_last(wide_ref[0, rows, :], weight_ref[0])
            total += contract_last(wide_ref[1, rows, :], weight_ref[1])
            total += contract_last(wide_ref[2, rows, :], weight_ref[2])
            spread = jnp.concatenate([jnp.zeros((3 * rank, LANES), jnp.float32), found], axis=0)
            values.append(total + spread.T)
        for place, out_ref in enumerate(out_refs):

            @pl.when(r == place)
            def _():
                for s in range(per_member):
                    out_ref[s * slot_len : (s + 1) * slot_len, :] = values[s]

        return 0

    lax.fori_loop(0, members, step, 0)


def sketch_kernel(rank, slot_len, per_member, len_ref, *refs):
    parts, out_ref, full_ref = refs[:-2], refs[-2], refs[-1]
    me = lax.axis_index("mp").astype(jnp.int32)
    lane = lax.broadcasted_iota(jnp.int32, (8, LANES), 1)
    for s in range(per_member):
        rows = slice(s * slot_len, (s + 1) * slot_len)
        total = parts[0][rows, :]
        for part in parts[1:]:
            total = total + part[rows, :]
        live = len_ref[me * per_member + s]
        position = lax.broadcasted_iota(jnp.int32, (slot_len, LANES), 0)
        share = 1.0 / jnp.full((slot_len, LANES), live, jnp.int32).astype(jnp.float32)
        weighted = total * jnp.where(position < live, share, 0.0)
        full_ref[s] = lax.dot_general(
            weighted, total, (((0,), (0,)), ((), ())), precision=highest, preferred_element_type=jnp.float32
        )
        for layer in range(2):
            source = 3 - layer
            unit = jnp.zeros((8, LANES), jnp.float32)
            for c in range(4):
                piece = full_ref[s, pl.ds(layer * rank + c, 8, stride=4), :]
                turned = pltpu.roll(piece, ((c - source) * rank) % LANES, 1)
                unit = jnp.where((lane >= c * rank) & (lane < (c + 1) * rank), turned, unit)
            out_ref[pl.ds((s * 2 + layer) * 8, 8), :] = unit


def swap_blocks(value, axis, width, index, count):
    size = value.shape[axis]
    place = lax.broadcasted_iota(jnp.int32, value.shape, axis)
    bit = 1
    while bit < count:
        shift = bit * width
        up = pltpu.roll(value, shift, axis)
        down = pltpu.roll(value, size - shift, axis)
        other = jnp.where((place // shift) % 2 == 1, up, down)
        value = jnp.where((index // bit) % 2 == 1, other, value)
        bit *= 2
    return value


def split_halves(ref, layer, first, count, chunk):
    wide = [ref[pl.ds(layer * 8 + first + j, count, stride=16), :] for j in range(chunk // LANES)]
    value = jnp.concatenate(wide, axis=1)
    high = value.astype(jnp.bfloat16)
    low = (value - high.astype(jnp.float32)).astype(jnp.bfloat16)
    return jnp.concatenate([high, low], axis=0)


def fold_rows(value):
    half = value.shape[0] // 2
    return value[:half] + value[half:]


def fold(value):
    half = value.shape[1] // 2
    value = fold_rows(value)
    return value[:, :half] + value[:, half:]


def own_kernel(mp, mine_ref, qmine_ref, qother_ref, both_ref, gram_ref, u_ref, norm_ref):
    me = lax.axis_index("mp").astype(jnp.int32)
    half = gram_ref.shape[1]
    columns = qmine_ref.shape[1] * qmine_ref.shape[3]
    chunk = qmine_ref.shape[4]
    for layer in range(2):
        square = jnp.zeros((2 * half, 2 * half), jnp.float32)
        mixed = [jnp.zeros((2 * half, columns), jnp.float32) for _ in range(2)]
        norms = [jnp.zeros((columns, LANES), jnp.float32) for _ in range(2)]
        for k in range(mp):
            both = split_halves(mine_ref, layer, (me ^ k) * (chunk // LANES), half, chunk)
            both_ref[layer, :, k * chunk : (k + 1) * chunk] = both
            square += contract_last(both, both)
            for side, ref in enumerate((qmine_ref, qother_ref)):
                query = ref[k, :, layer].reshape(columns, chunk)
                mixed[side] += contract_last(both, query)
                wide_query = query.astype(jnp.float32)
                squared = wide_query * wide_query
                for j in range(chunk // LANES):
                    norms[side] += squared[:, j * LANES : (j + 1) * LANES]
        gram_ref[layer] = fold(square)
        for side in range(2):
            u_ref[layer, :, side * columns : (side + 1) * columns] = fold_rows(mixed[side])
        norm_ref[layer] = lax.dot_general(
            jnp.ones((8, LANES), jnp.float32),
            jnp.concatenate(norms, axis=0),
            (((1,), (1,)), ((), ())),
            precision=highest,
            preferred_element_type=jnp.float32,
        )


def solve_kernel(
    mp, zs, per_member, examples, other_ref, both_ref, gram_ref, u_ref, norm_ref, qmine_ref, qother_ref, out_ref
):
    me = lax.axis_index("mp").astype(jnp.int32)
    mydp = lax.axis_index("dp").astype(jnp.int32)
    half = gram_ref.shape[1]
    columns = qmine_ref.shape[1] * qmine_ref.shape[3]
    chunk = qmine_ref.shape[4]
    scores = None
    for layer in range(2):
        square = jnp.zeros((2 * half, 2 * half), jnp.float32)
        cross = jnp.zeros((2 * half, 2 * half), jnp.float32)
        mixed = [jnp.zeros((2 * half, columns), jnp.float32) for _ in range(2)]
        for k in range(mp):
            both = split_halves(other_ref, layer, (me ^ k) * (chunk // LANES), half, chunk)
            square += contract_last(both, both)
            cross += contract_last(both_ref[layer, :, k * chunk : (k + 1) * chunk], both)
            for side, ref in enumerate((qmine_ref, qother_ref)):
                mixed[side] += contract_last(both, ref[k, :, layer].reshape(columns, chunk))
        cross = fold(cross)
        own_u = u_ref[layer]
        other_u = jnp.concatenate([fold_rows(m) for m in mixed], axis=1)
        u = jnp.concatenate([own_u, other_u], axis=0)
        dot = functools.partial(jnp.dot, precision=highest, preferred_element_type=jnp.float32)
        ku = jnp.concatenate(
            [dot(gram_ref[layer], own_u) + dot(cross, other_u), dot(cross.T, own_u) + dot(fold(square), other_u)],
            axis=0,
        )
        qq = norm_ref[layer][:1]
        uu = jnp.sum(u * u, axis=0, keepdims=True)
        uku = jnp.sum(u * ku, axis=0, keepdims=True)
        step0 = qq / (uu / examples + damping * qq + epsilon)
        alpha = 1.0 - damping * step0
        beta = -step0 / examples
        rr = jnp.maximum(alpha * alpha * qq + 2.0 * alpha * beta * uu + beta * beta * uku, 0.0)
        a = alpha + rr / (qq + epsilon)
        sd = a * u + beta * ku
        dd = jnp.maximum(a * a * qq + 2.0 * a * beta * uu + beta * beta * uku, 0.0)
        step1 = rr / (jnp.sum(sd * sd, axis=0, keepdims=True) / examples + damping * dd + epsilon)
        value = step0 * u + step1 * sd
        scores = value if scores is None else scores + value
    own = jnp.concatenate(
        [scores[k * zs * per_member : k * zs * per_member + per_member] for k in range(mp)], axis=0
    )
    own = swap_blocks(own, 0, per_member, me, mp)
    width = columns // zs
    own = jnp.concatenate(
        [own[:, (c * zs + z) * width : (c * zs + z + 1) * width] for z in range(zs) for c in range(2)], axis=1
    )
    out_ref[...] = swap_blocks(own, 1, width, mydp, 2 * zs)


def exchange(value, axis, count, unit=1):
    size = lax.axis_size(axis)
    return [value] + [
        lax.ppermute(value, axis, [(i, i ^ (k * unit)) for i in range(size)]) for k in range(1, count)
    ]


def fast_device(
    token_ids,
    lengths,
    embed_grads,
    vocab_basis,
    embed_basis,
    layer_inputs,
    layer_grads,
    input_basis,
    output_basis,
    queries,
):
    vocab_rows, rank = vocab_basis.shape
    seq_count = lengths.shape[0]
    token_count, features = embed_grads.shape
    slot_len = token_count // seq_count
    mp, dp = lax.axis_size("mp"), lax.axis_size("dp")
    zs = dp // 2
    per_member = seq_count // mp
    examples = seq_count * dp
    placed = lambda space, *values: [pltpu.with_memory_space_constraint(v, space) for v in values]
    whole = lambda n: [pl.BlockSpec(memory_space=pltpu.VMEM)] * n
    limit = pltpu.CompilerParams(vmem_limit_bytes=16 * 2**20)

    block = per_member * slot_len
    sent = pl.pallas_call(
        functools.partial(project_kernel, vocab_rows, rank, slot_len, per_member),
        out_shape=[pltpu.VMEM((block, LANES), jnp.float32)] * mp,
        in_specs=[pl.BlockSpec(memory_space=pl.ANY)] * 8,
        out_specs=whole(mp),
        scratch_shapes=[
            pltpu.VMEM((seq_count, slot_len), jnp.int32),
            pltpu.VMEM((rank, vocab_rows), jnp.bfloat16),
            pltpu.VMEM((3, token_count, features), jnp.bfloat16),
            pltpu.VMEM((3, LANES, features), jnp.bfloat16),
            pltpu.VMEM((2, seq_count, slot_len), jnp.int32),
            pltpu.SMEM((2, seq_count, slot_len), jnp.int32),
            pltpu.SemaphoreType.DMA((5,)),
            pltpu.SemaphoreType.DMA((3, mp)),
        ],
        compiler_params=limit,
        name="project",
    )(
        *placed(
            pltpu.HBM,
            token_ids.reshape(seq_count, slot_len),
            vocab_basis.T,
            embed_grads,
            layer_grads[0],
            layer_inputs[0],
            embed_basis.T,
            output_basis[0].T,
            input_basis[0].T,
        )
    )
    parts = [sent[0]]
    for k in range(1, mp):
        parts.append(lax.ppermute(sent[k], "mp", [(i, i ^ k) for i in range(mp)]))

    pieces = exchange(queries.transpose(0, 2, 1), "dp", zs, 2)
    rows = per_member * 2 * 8
    units = pl.pallas_call(
        functools.partial(sketch_kernel, rank, slot_len, per_member),
        out_shape=pltpu.VMEM((rows, LANES), jnp.float32),
        in_specs=[pl.BlockSpec(memory_space=pltpu.SMEM)] + whole(mp),
        out_specs=whole(1)[0],
        scratch_shapes=[pltpu.VMEM((per_member, LANES, LANES), jnp.float32)],
        compiler_params=limit,
        name="sketch",
    )(lengths, *placed(pltpu.VMEM, *parts))
    along_z = jnp.concatenate(exchange(units, "dp", zs, 2))
    pieces = lax.optimization_barrier((*pieces, units))[:-1]
    qall = jnp.stack(exchange(jnp.stack(pieces), "mp", mp))
    qcore = exchange(qall, "dp", 2)[1]
    mine = jnp.concatenate(exchange(along_z, "mp", mp))
    other = exchange(mine, "dp", 2)[1]
    half = mp * zs * per_member
    columns = queries.shape[2] * dp
    sketch_len = rank * rank
    own_terms = pl.pallas_call(
        functools.partial(own_kernel, mp),
        out_shape=[
            pltpu.VMEM((2, 2 * half, sketch_len), jnp.bfloat16),
            pltpu.VMEM((2, half, half), jnp.float32),
            pltpu.VMEM((2, half, columns), jnp.float32),
            pltpu.VMEM((2, 8, columns), jnp.float32),
        ],
        in_specs=whole(3),
        out_specs=whole(4),
        compiler_params=limit,
        name="own",
    )(*placed(pltpu.VMEM, mine, qall, qcore))
    return pl.pallas_call(
        functools.partial(solve_kernel, mp, zs, per_member, examples),
        out_shape=jax.ShapeDtypeStruct((seq_count, columns), jnp.float32),
        in_specs=whole(7),
        out_specs=whole(1)[0],
        compiler_params=limit,
        name="solve",
    )(*placed(pltpu.VMEM, other, *own_terms, qall, qcore))


def power_of_two(n):
    return n & (n - 1) == 0


def solution(mesh):
    placed = (
        P("dp"),
        P("dp"),
        P("dp", "mp"),
        P("mp", None),
        P("mp", None),
        P(None, "dp", "mp"),
        P(None, "dp", "mp"),
        P(None, "mp", None),
        P(None, "mp", None),
        P(None, "mp", "dp"),
    )

    def per_device(*args):
        mp, dp = mesh.shape["mp"], mesh.shape["dp"]
        token_ids, lengths, layer_inputs, queries = args[0], args[1], args[5], args[9]
        seq_count, rank = lengths.shape[0], args[3].shape[1]
        fits = (
            layer_inputs.shape[0] == 1
            and token_ids.shape[0] == seq_count * LANES
            and rank * 4 == LANES
            and seq_count % 8 == 0
            and seq_count % mp == 0
            and power_of_two(mp)
            and power_of_two(dp)
            and dp % 2 == 0
            and queries.shape[1] % LANES == 0
            and queries.shape[2] % 16 == 0
            and queries.shape[2] * dp // 2 == LANES
        )
        if not fits:
            return general_device(*args)
        return fast_device(*args)

    return jax.shard_map(per_device, mesh=mesh, in_specs=placed, out_specs=P("dp", None), check_vma=False)
```

```python
import functools

import jax
import jax.numpy as jnp
from jax import lax
from jax.experimental import pallas as pl
from jax.experimental.pallas import tpu as pltpu
from jax.sharding import PartitionSpec as P


ITERS = 2
LANES = 128
AHEAD = 1

damping = 0.01
epsilon = 1e-06
highest = lax.Precision.HIGHEST


def solve_columns(right_side, apply_operator, column_norm, column_curve):
    solution = jnp.zeros_like(right_side)
    residual = right_side
    direction = right_side
    norm_now = column_norm(residual)
    for _ in range(ITERS):
        images = apply_operator(direction)
        step_size = norm_now / (column_curve(direction, images) + epsilon)
        solution = solution + step_size[:, None, :] * direction
        residual = residual - step_size[:, None, :] * images
        norm_next = column_norm(residual)
        direction = residual + (norm_next / (norm_now + epsilon))[:, None, :] * direction
        norm_now = norm_next
    return solution


def general_device(
    token_ids,
    lengths,
    embed_grads,
    vocab_basis,
    embed_basis,
    layer_inputs,
    layer_grads,
    input_basis,
    output_basis,
    queries,
):
    vocab_rows = vocab_basis.shape[0]
    basis_rank = embed_basis.shape[1]
    layer_count = layer_inputs.shape[0] + 1
    seq_count = lengths.shape[0]
    token_count = token_ids.shape[0]
    slot_len = token_count // seq_count
    sketch_len = basis_rank * basis_rank
    mp_index = lax.axis_index("mp")
    local_ids = token_ids - mp_index * vocab_rows
    inside = (local_ids >= 0) & (local_ids < vocab_rows)
    looked = jnp.take(vocab_basis, jnp.clip(local_ids, 0, vocab_rows - 1), axis=0)
    pieces = [
        jnp.dot(embed_grads, embed_basis, preferred_element_type=jnp.float32),
        jnp.where(inside[:, None], looked.astype(jnp.float32), 0.0),
    ]
    for layer in range(layer_count - 1):
        pieces.append(jnp.dot(layer_grads[layer], output_basis[layer], preferred_element_type=jnp.float32))
        pieces.append(jnp.dot(layer_inputs[layer], input_basis[layer], preferred_element_type=jnp.float32))
    projected = jnp.concatenate(pieces, axis=1)
    inverse_len = 1.0 / lengths.astype(jnp.float32)
    summed = lax.psum(projected, "mp")
    layout = summed.reshape(seq_count, slot_len, layer_count, 2, basis_rank)
    position = jnp.arange(slot_len, dtype=jnp.int32)
    weights = jnp.where(position[None, :] < lengths[:, None], inverse_len[:, None], 0.0)
    weighted = layout[:, :, :, 0, :] * weights[:, :, None, None]
    sketches = jnp.einsum(
        "stli,stlj->lsij", weighted, layout[:, :, :, 1, :], precision=highest
    ).reshape(layer_count, seq_count, sketch_len)
    examples = seq_count * lax.axis_size("dp")
    targets = lax.all_gather(queries, "dp", axis=2, tiled=True)
    everyone = lax.all_gather(sketches, "dp", axis=1, tiled=True)
    columns = lax.all_to_all(targets, "mp", split_axis=2, concat_axis=1, tiled=True)

    def apply_sketch(direction):
        inner_sums = jnp.einsum("lek,lkq->leq", everyone, direction, precision=highest)
        back_proj = jnp.einsum("lek,leq->lkq", everyone, inner_sums, precision=highest)
        return back_proj / examples + damping * direction

    def local_norm(residual):
        return jnp.sum(residual * residual, axis=1)

    def local_curve(direction, images):
        return jnp.sum(direction * images, axis=1)

    solution = solve_columns(columns.astype(jnp.float32), apply_sketch, local_norm, local_curve)
    partial_value = jnp.einsum("lek,lkq->eq", sketches, solution, precision=highest)
    return lax.all_gather(partial_value, "mp", axis=1, tiled=True)


def contract_last(left, right):
    return lax.dot_general(left, right, (((1,), (1,)), ((), ())), preferred_element_type=jnp.float32)


def project_kernel(
    vocab_rows,
    rank,
    slot_len,
    per_member,
    ids_any,
    len_any,
    table_any,
    grad0_any,
    grad1_any,
    input1_any,
    basis0_any,
    basis1_any,
    basis2_any,
    *refs,
):
    out_refs = refs[:-9]
    ids_ref, len_ref, table_ref, wide_ref, weight_ref, place_ref, scalar_ref = refs[-9:-2]
    small_sem, wide_sem = refs[-2:]
    members = len(out_refs)
    me = lax.axis_index("mp").astype(jnp.int32)
    offset = me * vocab_rows
    main = vocab_rows // LANES
    block = per_member * slot_len

    def rows_of(r):
        return pl.ds(pl.multiple_of((me ^ r) * block, block), block)

    def wide_copy(k, r):
        source = (grad0_any, grad1_any, input1_any)[k]
        return pltpu.make_async_copy(source.at[rows_of(r), :], wide_ref.at[k, rows_of(r), :], wide_sem.at[k, r])

    ids_copy = pltpu.make_async_copy(ids_any, ids_ref, small_sem.at[0])
    len_copy = pltpu.make_async_copy(len_any, len_ref, small_sem.at[5])
    table_copy = pltpu.make_async_copy(table_any, table_ref, small_sem.at[1])
    basis_copies = [
        pltpu.make_async_copy(basis, weight_ref.at[k, pl.ds(k * rank, rank), :], small_sem.at[2 + k])
        for k, basis in enumerate((basis0_any, basis1_any, basis2_any))
    ]
    ids_copy.start()
    table_copy.start()
    len_copy.start()
    for copy in basis_copies:
        copy.start()
    for r in range(AHEAD):
        for k in range(3):
            wide_copy(k, r).start()
    for k in range(3):
        if k:
            weight_ref[k, : k * rank, :] = jnp.zeros((k * rank, weight_ref.shape[2]), jnp.bfloat16)
        weight_ref[k, (k + 1) * rank :, :] = jnp.zeros((LANES - (k + 1) * rank, weight_ref.shape[2]), jnp.bfloat16)
    ids_copy.wait()
    local = ids_ref[...] - offset
    position = lax.broadcasted_iota(jnp.int32, local.shape, 1)
    place_ref[...] = jnp.clip(local >> 7, 0, main - 1) * LANES + ((position - local) & (LANES - 1))
    scalar_copy = pltpu.make_async_copy(place_ref, scalar_ref, small_sem.at[0])
    scalar_copy.start()
    scalar_copy.wait()
    len_copy.wait()
    for copy in basis_copies:
        copy.wait()
    table_copy.wait()
    for r in range(AHEAD, members):
        for k in range(3):
            wide_copy(k, r).start()

    lane = lax.broadcasted_iota(jnp.int32, (rank, LANES), 1)
    row = lax.broadcasted_iota(jnp.int32, (slot_len, LANES), 0)
    column = lax.broadcasted_iota(jnp.int32, (slot_len, LANES), 1)
    tail = vocab_rows - main * LANES

    def step(r, _):
        for k in range(3):
            wide_copy(k, r).wait()
        values = []
        for s in range(per_member):
            seq = (me ^ r) * per_member + s
            found = jnp.zeros((rank, LANES), jnp.float32)
            for t in range(slot_len):
                word = scalar_ref[seq, t]
                block = table_ref[:, pl.ds(pl.multiple_of(word & -LANES, LANES), LANES)].astype(jnp.float32)
                found = jnp.where(lane == t, pltpu.roll(block, word & (LANES - 1), 1), found)
            mine = ids_ref[pl.ds(seq, 1), :] - offset
            found = jnp.where((mine >= 0) & (mine < main * LANES), found, 0.0)
            if tail:
                sub = lax.broadcasted_iota(jnp.int32, (tail, LANES), 0)
                pick = jnp.where(mine - main * LANES == sub, 1.0, 0.0).astype(jnp.bfloat16)
                found += jnp.dot(table_ref[:, main * LANES :], pick, preferred_element_type=jnp.float32)
            rows = pl.ds(pl.multiple_of(seq * slot_len, slot_len), slot_len)
            total = contract_last(wide_ref[0, rows, :], weight_ref[0])
            total += contract_last(wide_ref[1, rows, :], weight_ref[1])
            total += contract_last(wide_ref[2, rows, :], weight_ref[2])
            live = len_ref[seq]
            share = jnp.where(row < live, 1.0 / jnp.full(row.shape, live, jnp.int32).astype(jnp.float32), 0.0)
            spread = jnp.concatenate([jnp.zeros((3 * rank, LANES), jnp.float32), found], axis=0)
            values.append(total * jnp.where(column < 2 * rank, share, 1.0) + spread.T)
        for place, out_ref in enumerate(out_refs):

            @pl.when(r == place)
            def _():
                for s in range(per_member):
                    out_ref[s * slot_len : (s + 1) * slot_len, :] = values[s]

        return 0

    lax.fori_loop(0, members, step, 0)


def split(value):
    high = value.astype(jnp.bfloat16)
    return high, (value - high.astype(jnp.float32)).astype(jnp.bfloat16)


def fold_rows(value):
    half = value.shape[0] // 2
    return value[:half] + value[half:]


def sketch_kernel(rank, slot_len, per_member, *refs):
    parts, out_ref, full_ref = refs[:-2], refs[-2], refs[-1]
    lane = lax.broadcasted_iota(jnp.int32, (8, LANES), 1)
    for s in range(per_member):
        rows = slice(s * slot_len, (s + 1) * slot_len)
        total = parts[0][rows, :]
        for part in parts[1:]:
            total = total + part[rows, :]
        grads_high, grads_low = split(total[:, : 2 * rank])
        high, low = split(total)
        product = lax.dot_general(
            jnp.concatenate([grads_high, grads_low], axis=1),
            jnp.concatenate([high, low], axis=1),
            (((0,), (0,)), ((), ())),
            preferred_element_type=jnp.float32,
        )
        full_ref[s] = fold_rows(product[:, :LANES] + product[:, LANES:])
        for layer in range(2):
            source = 3 - layer
            unit = jnp.zeros((8, LANES), jnp.float32)
            for c in range(4):
                piece = full_ref[s, pl.ds(layer * rank + c, 8, stride=4), :]
                turned = pltpu.roll(piece, ((c - source) * rank) % LANES, 1)
                unit = jnp.where((lane >= c * rank) & (lane < (c + 1) * rank), turned, unit)
            out_ref[pl.ds((s * 2 + layer) * 8, 8), :] = unit


def swap_blocks(value, axis, width, index, count):
    size = value.shape[axis]
    place = lax.broadcasted_iota(jnp.int32, value.shape, axis)
    bit = 1
    while bit < count:
        shift = bit * width
        up = pltpu.roll(value, shift, axis)
        down = pltpu.roll(value, size - shift, axis)
        other = jnp.where((place // shift) % 2 == 1, up, down)
        value = jnp.where((index // bit) % 2 == 1, other, value)
        bit *= 2
    return value


def split_rows(ref, layer, first, count, chunk):
    wide = [ref[pl.ds(layer * 8 + first + j, count, stride=16), :] for j in range(chunk // LANES)]
    return jnp.concatenate(split(jnp.concatenate(wide, axis=1)), axis=0)


def own_kernel(mp, mine_ref, qmine_ref, qother_ref, both_ref, u_ref, norm_ref):
    me = lax.axis_index("mp").astype(jnp.int32)
    half = u_ref.shape[1]
    columns = qmine_ref.shape[1] * qmine_ref.shape[3]
    chunk = qmine_ref.shape[4]
    for layer in range(2):
        mixed = [jnp.zeros((2 * half, columns), jnp.float32) for _ in range(2)]
        norms = [jnp.zeros((columns, LANES), jnp.float32) for _ in range(2)]
        for k in range(mp):
            both = split_rows(mine_ref, layer, (me ^ k) * (chunk // LANES), half, chunk)
            both_ref[layer, :, k * chunk : (k + 1) * chunk] = both
            for side in range(2):
                query = (qmine_ref, qother_ref)[side][k, :, layer].reshape(columns, chunk)
                mixed[side] += contract_last(both, query)
                wide_query = query.astype(jnp.float32)
                squared = wide_query * wide_query
                for j in range(chunk // LANES):
                    norms[side] += squared[:, j * LANES : (j + 1) * LANES]
        for side in range(2):
            u_ref[layer, :, side * columns : (side + 1) * columns] = fold_rows(mixed[side])
        norm_ref[layer] = lax.dot_general(
            jnp.ones((8, LANES), jnp.float32),
            jnp.concatenate(norms, axis=0),
            (((1,), (1,)), ((), ())),
            precision=highest,
            preferred_element_type=jnp.float32,
        )


def solve_kernel(
    mp, zs, per_member, examples, other_ref, both_ref, u_ref, norm_ref, qmine_ref, qother_ref, out_ref
):
    me = lax.axis_index("mp").astype(jnp.int32)
    mydp = lax.axis_index("dp").astype(jnp.int32)
    half = u_ref.shape[1]
    columns = qmine_ref.shape[1] * qmine_ref.shape[3]
    chunk = qmine_ref.shape[4]
    scores = None
    for layer in range(2):
        square = jnp.zeros((4 * half, 4 * half), jnp.float32)
        mixed = [jnp.zeros((2 * half, columns), jnp.float32) for _ in range(2)]
        for k in range(mp):
            other = split_rows(other_ref, layer, (me ^ k) * (chunk // LANES), half, chunk)
            every = jnp.concatenate([both_ref[layer, :, k * chunk : (k + 1) * chunk], other], axis=0)
            square += contract_last(every, every)
            for side in range(2):
                query = (qmine_ref, qother_ref)[side][k, :, layer].reshape(columns, chunk)
                mixed[side] += contract_last(other, query)
        gram = jnp.concatenate([fold_rows(square[: 2 * half]), fold_rows(square[2 * half :])], axis=0)
        own_u = u_ref[layer]
        other_u = jnp.concatenate([fold_rows(m) for m in mixed], axis=1)
        u = jnp.concatenate([own_u, other_u], axis=0)
        u_high, u_low = split(jnp.concatenate([own_u, own_u, other_u, other_u], axis=0))
        gram_high, gram_low = split(gram)
        terms = jnp.dot(
            jnp.concatenate([gram_high, gram_low], axis=0), u_high, preferred_element_type=jnp.float32
        )
        ku = fold_rows(terms) + jnp.dot(gram_high, u_low, preferred_element_type=jnp.float32)
        qq = norm_ref[layer][:1]
        uu = jnp.sum(u * u, axis=0, keepdims=True)
        uku = jnp.sum(u * ku, axis=0, keepdims=True)
        step0 = qq / (uu / examples + damping * qq + epsilon)
        alpha = 1.0 - damping * step0
        beta = -step0 / examples
        rr = jnp.maximum(alpha * alpha * qq + 2.0 * alpha * beta * uu + beta * beta * uku, 0.0)
        a = alpha + rr / (qq + epsilon)
        sd = a * u + beta * ku
        dd = jnp.maximum(a * a * qq + 2.0 * a * beta * uu + beta * beta * uku, 0.0)
        step1 = rr / (jnp.sum(sd * sd, axis=0, keepdims=True) / examples + damping * dd + epsilon)

        def own_rows(value):
            starts = [k * zs * per_member for k in range(mp)]
            return jnp.concatenate([value[start : start + per_member] for start in starts], axis=0)

        value = step0 * own_rows(u) + step1 * own_rows(sd)
        scores = value if scores is None else scores + value
    own = swap_blocks(scores, 0, per_member, me, mp)
    width = columns // zs
    places = [(c * zs + z) * width for z in range(zs) for c in range(2)]
    own = jnp.concatenate([own[:, place : place + width] for place in places], axis=1)
    out_ref[...] = swap_blocks(own, 1, width, mydp, 2 * zs)


def exchange_z(value, zs):
    return [value] + [lax.ppermute(value, "dp", [(i, i ^ (2 * k)) for i in range(2 * zs)]) for k in range(1, zs)]


def exchange_mp(value, mp):
    return [value] + [lax.ppermute(value, "mp", [(i, i ^ k) for i in range(mp)]) for k in range(1, mp)]


def exchange_core(value, dp):
    return lax.ppermute(value, "dp", [(i, i ^ 1) for i in range(dp)])


def fast_device(
    token_ids,
    lengths,
    embed_grads,
    vocab_basis,
    embed_basis,
    layer_inputs,
    layer_grads,
    input_basis,
    output_basis,
    queries,
):
    vocab_rows, rank = vocab_basis.shape
    seq_count = lengths.shape[0]
    token_count, features = embed_grads.shape
    slot_len = token_count // seq_count
    mp, dp = lax.axis_size("mp"), lax.axis_size("dp")
    zs = dp // 2
    per_member = seq_count // mp
    examples = seq_count * dp
    placed = lambda space, *values: [pltpu.with_memory_space_constraint(v, space) for v in values]
    whole = lambda n: [pl.BlockSpec(memory_space=pltpu.VMEM)] * n
    limit = pltpu.CompilerParams(vmem_limit_bytes=16 * 2**20)

    block = per_member * slot_len
    sent = pl.pallas_call(
        functools.partial(project_kernel, vocab_rows, rank, slot_len, per_member),
        out_shape=[pltpu.VMEM((block, LANES), jnp.float32)] * mp,
        in_specs=[pl.BlockSpec(memory_space=pl.ANY)] * 9,
        out_specs=whole(mp),
        scratch_shapes=[
            pltpu.VMEM((seq_count, slot_len), jnp.int32),
            pltpu.SMEM((seq_count,), jnp.int32),
            pltpu.VMEM((rank, vocab_rows), jnp.bfloat16),
            pltpu.VMEM((3, token_count, features), jnp.bfloat16),
            pltpu.VMEM((3, LANES, features), jnp.bfloat16),
            pltpu.VMEM((seq_count, slot_len), jnp.int32),
            pltpu.SMEM((seq_count, slot_len), jnp.int32),
            pltpu.SemaphoreType.DMA((6,)),
            pltpu.SemaphoreType.DMA((3, mp)),
        ],
        compiler_params=limit,
        name="project",
    )(
        *placed(
            pltpu.HBM,
            token_ids.reshape(seq_count, slot_len),
            lengths,
            vocab_basis.T,
            embed_grads,
            layer_grads[0],
            layer_inputs[0],
            embed_basis.T,
            output_basis[0].T,
            input_basis[0].T,
        )
    )
    parts = [sent[0]]
    for k in range(1, mp):
        parts.append(lax.ppermute(sent[k], "mp", [(i, i ^ k) for i in range(mp)]))

    pieces = exchange_z(queries.transpose(0, 2, 1), zs)
    rows = per_member * 2 * 8
    units = pl.pallas_call(
        functools.partial(sketch_kernel, rank, slot_len, per_member),
        out_shape=pltpu.VMEM((rows, LANES), jnp.float32),
        in_specs=whole(mp),
        out_specs=whole(1)[0],
        scratch_shapes=[pltpu.VMEM((per_member, 2 * rank, LANES), jnp.float32)],
        compiler_params=limit,
        name="sketch",
    )(*placed(pltpu.VMEM, *parts))
    along_z = jnp.concatenate(exchange_z(units, zs))
    pieces = lax.optimization_barrier((*pieces, units))[:-1]
    qall = jnp.stack(exchange_mp(jnp.stack(pieces), mp))
    qcore = exchange_core(qall, dp)
    mine = jnp.concatenate(exchange_mp(along_z, mp))
    other = exchange_core(mine, dp)
    half = mp * zs * per_member
    columns = queries.shape[2] * dp
    sketch_len = rank * rank
    own_terms = pl.pallas_call(
        functools.partial(own_kernel, mp),
        out_shape=[
            pltpu.VMEM((2, 2 * half, sketch_len), jnp.bfloat16),
            pltpu.VMEM((2, half, columns), jnp.float32),
            pltpu.VMEM((2, 8, columns), jnp.float32),
        ],
        in_specs=whole(3),
        out_specs=whole(3),
        compiler_params=limit,
        name="own",
    )(*placed(pltpu.VMEM, mine, qall, qcore))
    return pl.pallas_call(
        functools.partial(solve_kernel, mp, zs, per_member, examples),
        out_shape=jax.ShapeDtypeStruct((seq_count, columns), jnp.float32),
        in_specs=whole(6),
        out_specs=whole(1)[0],
        compiler_params=limit,
        name="solve",
    )(*placed(pltpu.VMEM, other, *own_terms, qall, qcore))


def power_of_two(n):
    return n & (n - 1) == 0


def solution(mesh):
    placed = (
        P("dp"),
        P("dp"),
        P("dp", "mp"),
        P("mp", None),
        P("mp", None),
        P(None, "dp", "mp"),
        P(None, "dp", "mp"),
        P(None, "mp", None),
        P(None, "mp", None),
        P(None, "mp", "dp"),
    )

    def per_device(*args):
        mp, dp = mesh.shape["mp"], mesh.shape["dp"]
        token_ids, lengths, layer_inputs, queries = args[0], args[1], args[5], args[9]
        seq_count, rank = lengths.shape[0], args[3].shape[1]
        fits = (
            layer_inputs.shape[0] == 1
            and token_ids.shape[0] == seq_count * LANES
            and rank * 4 == LANES
            and seq_count % 8 == 0
            and seq_count % mp == 0
            and power_of_two(mp)
            and power_of_two(dp)
            and dp % 2 == 0
            and queries.shape[1] % LANES == 0
            and queries.shape[2] % 16 == 0
            and queries.shape[2] * dp // 2 == LANES
        )
        if not fits:
            return general_device(*args)
        return fast_device(*args)

    return jax.shard_map(per_device, mesh=mesh, in_specs=placed, out_specs=P("dp", None), check_vma=False)
```

```python
import functools

import jax
import jax.numpy as jnp
from jax import lax
from jax.experimental import pallas as pl
from jax.experimental.pallas import tpu as pltpu
from jax.sharding import PartitionSpec as P


ITERS = 2
LANES = 128
AHEAD = 1

damping = 0.01
epsilon = 1e-06
highest = lax.Precision.HIGHEST


def solve_columns(right_side, apply_operator, column_norm, column_curve):
    solution = jnp.zeros_like(right_side)
    residual = right_side
    direction = right_side
    norm_now = column_norm(residual)
    for _ in range(ITERS):
        images = apply_operator(direction)
        step_size = norm_now / (column_curve(direction, images) + epsilon)
        solution = solution + step_size[:, None, :] * direction
        residual = residual - step_size[:, None, :] * images
        norm_next = column_norm(residual)
        direction = residual + (norm_next / (norm_now + epsilon))[:, None, :] * direction
        norm_now = norm_next
    return solution


def general_device(
    token_ids,
    lengths,
    embed_grads,
    vocab_basis,
    embed_basis,
    layer_inputs,
    layer_grads,
    input_basis,
    output_basis,
    queries,
):
    vocab_rows = vocab_basis.shape[0]
    basis_rank = embed_basis.shape[1]
    layer_count = layer_inputs.shape[0] + 1
    seq_count = lengths.shape[0]
    token_count = token_ids.shape[0]
    slot_len = token_count // seq_count
    sketch_len = basis_rank * basis_rank
    mp_index = lax.axis_index("mp")
    local_ids = token_ids - mp_index * vocab_rows
    inside = (local_ids >= 0) & (local_ids < vocab_rows)
    looked = jnp.take(vocab_basis, jnp.clip(local_ids, 0, vocab_rows - 1), axis=0)
    pieces = [
        jnp.dot(embed_grads, embed_basis, preferred_element_type=jnp.float32),
        jnp.where(inside[:, None], looked.astype(jnp.float32), 0.0),
    ]
    for layer in range(layer_count - 1):
        pieces.append(jnp.dot(layer_grads[layer], output_basis[layer], preferred_element_type=jnp.float32))
        pieces.append(jnp.dot(layer_inputs[layer], input_basis[layer], preferred_element_type=jnp.float32))
    projected = jnp.concatenate(pieces, axis=1)
    inverse_len = 1.0 / lengths.astype(jnp.float32)
    summed = lax.psum(projected, "mp")
    layout = summed.reshape(seq_count, slot_len, layer_count, 2, basis_rank)
    position = jnp.arange(slot_len, dtype=jnp.int32)
    weights = jnp.where(position[None, :] < lengths[:, None], inverse_len[:, None], 0.0)
    weighted = layout[:, :, :, 0, :] * weights[:, :, None, None]
    sketches = jnp.einsum(
        "stli,stlj->lsij", weighted, layout[:, :, :, 1, :], precision=highest
    ).reshape(layer_count, seq_count, sketch_len)
    examples = seq_count * lax.axis_size("dp")
    targets = lax.all_gather(queries, "dp", axis=2, tiled=True)
    everyone = lax.all_gather(sketches, "dp", axis=1, tiled=True)
    columns = lax.all_to_all(targets, "mp", split_axis=2, concat_axis=1, tiled=True)

    def apply_sketch(direction):
        inner_sums = jnp.einsum("lek,lkq->leq", everyone, direction, precision=highest)
        back_proj = jnp.einsum("lek,leq->lkq", everyone, inner_sums, precision=highest)
        return back_proj / examples + damping * direction

    def local_norm(residual):
        return jnp.sum(residual * residual, axis=1)

    def local_curve(direction, images):
        return jnp.sum(direction * images, axis=1)

    solution = solve_columns(columns.astype(jnp.float32), apply_sketch, local_norm, local_curve)
    partial_value = jnp.einsum("lek,lkq->eq", sketches, solution, precision=highest)
    return lax.all_gather(partial_value, "mp", axis=1, tiled=True)


def contract_last(left, right):
    return lax.dot_general(left, right, (((1,), (1,)), ((), ())), preferred_element_type=jnp.float32)


def project_kernel(
    vocab_rows,
    rank,
    slot_len,
    per_member,
    ids_any,
    len_any,
    table_any,
    grad0_any,
    grad1_any,
    input1_any,
    basis0_any,
    basis1_any,
    basis2_any,
    *refs,
):
    out_refs = refs[:-9]
    ids_ref, len_ref, table_ref, wide_ref, weight_ref, place_ref, scalar_ref = refs[-9:-2]
    small_sem, wide_sem = refs[-2:]
    members = len(out_refs)
    me = lax.axis_index("mp").astype(jnp.int32)
    offset = me * vocab_rows
    main = vocab_rows // LANES
    block = per_member * slot_len

    def rows_of(r):
        return pl.ds(pl.multiple_of((me ^ r) * block, block), block)

    def wide_copy(k, r):
        source = (grad0_any, grad1_any, input1_any)[k]
        return pltpu.make_async_copy(source.at[rows_of(r), :], wide_ref.at[k, rows_of(r), :], wide_sem.at[k, r])

    ids_copy = pltpu.make_async_copy(ids_any, ids_ref, small_sem.at[0])
    len_copy = pltpu.make_async_copy(len_any, len_ref, small_sem.at[5])
    table_copy = pltpu.make_async_copy(table_any, table_ref, small_sem.at[1])
    basis_copies = [
        pltpu.make_async_copy(basis, weight_ref.at[k, pl.ds(k * rank, rank), :], small_sem.at[2 + k])
        for k, basis in enumerate((basis0_any, basis1_any, basis2_any))
    ]
    ids_copy.start()
    table_copy.start()
    len_copy.start()
    for copy in basis_copies:
        copy.start()
    for r in range(AHEAD):
        for k in range(3):
            wide_copy(k, r).start()
    for k in range(3):
        if k:
            weight_ref[k, : k * rank, :] = jnp.zeros((k * rank, weight_ref.shape[2]), jnp.bfloat16)
        weight_ref[k, (k + 1) * rank :, :] = jnp.zeros((LANES - (k + 1) * rank, weight_ref.shape[2]), jnp.bfloat16)
    ids_copy.wait()
    local = ids_ref[...] - offset
    position = lax.broadcasted_iota(jnp.int32, local.shape, 1)
    place_ref[...] = jnp.clip(local >> 7, 0, main - 1) * LANES + ((position - local) & (LANES - 1))
    scalar_copy = pltpu.make_async_copy(place_ref, scalar_ref, small_sem.at[0])
    scalar_copy.start()
    scalar_copy.wait()
    len_copy.wait()
    for copy in basis_copies:
        copy.wait()
    table_copy.wait()
    for r in range(AHEAD, members):
        for k in range(3):
            wide_copy(k, r).start()

    lane = lax.broadcasted_iota(jnp.int32, (rank, LANES), 1)
    row = lax.broadcasted_iota(jnp.int32, (slot_len, LANES), 0)
    column = lax.broadcasted_iota(jnp.int32, (slot_len, LANES), 1)
    tail = vocab_rows - main * LANES

    def step(r, _):
        for k in range(3):
            wide_copy(k, r).wait()
        values = []
        for s in range(per_member):
            seq = (me ^ r) * per_member + s
            found = jnp.zeros((rank, LANES), jnp.float32)
            for t in range(slot_len):
                word = scalar_ref[seq, t]
                block = table_ref[:, pl.ds(pl.multiple_of(word & -LANES, LANES), LANES)].astype(jnp.float32)
                found = jnp.where(lane == t, pltpu.roll(block, word & (LANES - 1), 1), found)
            mine = ids_ref[pl.ds(seq, 1), :] - offset
            found = jnp.where((mine >= 0) & (mine < main * LANES), found, 0.0)
            if tail:
                sub = lax.broadcasted_iota(jnp.int32, (tail, LANES), 0)
                pick = jnp.where(mine - main * LANES == sub, 1.0, 0.0).astype(jnp.bfloat16)
                found += jnp.dot(table_ref[:, main * LANES :], pick, preferred_element_type=jnp.float32)
            rows = pl.ds(pl.multiple_of(seq * slot_len, slot_len), slot_len)
            total = contract_last(wide_ref[0, rows, :], weight_ref[0])
            total += contract_last(wide_ref[1, rows, :], weight_ref[1])
            total += contract_last(wide_ref[2, rows, :], weight_ref[2])
            live = len_ref[seq]
            share = jnp.where(row < live, 1.0 / jnp.full(row.shape, live, jnp.int32).astype(jnp.float32), 0.0)
            spread = jnp.concatenate([jnp.zeros((3 * rank, LANES), jnp.float32), found], axis=0)
            values.append(total * jnp.where(column < 2 * rank, share, 1.0) + spread.T)
        for place, out_ref in enumerate(out_refs):

            @pl.when(r == place)
            def _():
                for s in range(per_member):
                    out_ref[s * slot_len : (s + 1) * slot_len, :] = values[s]

        return 0

    lax.fori_loop(0, members, step, 0)


def split(value):
    high = value.astype(jnp.bfloat16)
    return high, (value - high.astype(jnp.float32)).astype(jnp.bfloat16)


def fold_rows(value):
    half = value.shape[0] // 2
    return value[:half] + value[half:]


def sketch_kernel(rank, slot_len, per_member, *refs):
    parts, out_ref, full_ref = refs[:-2], refs[-2], refs[-1]
    lane = lax.broadcasted_iota(jnp.int32, (8, LANES), 1)
    for s in range(per_member):
        rows = slice(s * slot_len, (s + 1) * slot_len)
        total = parts[0][rows, :]
        for part in parts[1:]:
            total = total + part[rows, :]
        grads_high, grads_low = split(total[:, : 2 * rank])
        high, low = split(total)
        product = lax.dot_general(
            jnp.concatenate([grads_high, grads_low], axis=1),
            jnp.concatenate([high, low], axis=1),
            (((0,), (0,)), ((), ())),
            preferred_element_type=jnp.float32,
        )
        full_ref[s] = fold_rows(product[:, :LANES] + product[:, LANES:])
        for layer in range(2):
            source = 3 - layer
            unit = jnp.zeros((8, LANES), jnp.float32)
            for c in range(4):
                piece = full_ref[s, pl.ds(layer * rank + c, 8, stride=4), :]
                turned = pltpu.roll(piece, ((c - source) * rank) % LANES, 1)
                unit = jnp.where((lane >= c * rank) & (lane < (c + 1) * rank), turned, unit)
            out_ref[pl.ds((s * 2 + layer) * 8, 8), :] = unit


def split_rows(ref, layer, first, count, chunk):
    wide = [ref[pl.ds(layer * 8 + first + j, count, stride=16), :] for j in range(chunk // LANES)]
    return jnp.concatenate(split(jnp.concatenate(wide, axis=1)), axis=0)


def own_kernel(mp, zs, mine_ref, qmine_ref, qother_ref, both_ref, u_ref, norm_ref, query_ref):
    me = lax.axis_index("mp").astype(jnp.int32)
    mydp = lax.axis_index("dp").astype(jnp.int32)
    half, columns = u_ref.shape[1:]
    width, chunk = qmine_ref.shape[3:]
    for layer in range(2):
        mixed = jnp.zeros((2 * half, columns), jnp.float32)
        norms = jnp.zeros((columns, LANES), jnp.float32)
        for k in range(mp):
            both = split_rows(mine_ref, layer, (me ^ k) * (chunk // LANES), half, chunk)
            both_ref[layer, :, k * chunk : (k + 1) * chunk] = both
            for place in range(2 * zs):
                away = (mydp // 2) ^ (place // 2)
                query_ref[layer, k, place * width : (place + 1) * width, :] = jnp.where(
                    mydp % 2 == place % 2, qmine_ref[k, away, layer], qother_ref[k, away, layer]
                )
            query = query_ref[layer, k]
            mixed += contract_last(both, query)
            wide_query = query.astype(jnp.float32)
            squared = wide_query * wide_query
            for j in range(chunk // LANES):
                norms += squared[:, j * LANES : (j + 1) * LANES]
        u_ref[layer] = fold_rows(mixed)
        norm_ref[layer] = lax.dot_general(
            jnp.ones((8, LANES), jnp.float32),
            norms,
            (((1,), (1,)), ((), ())),
            precision=highest,
            preferred_element_type=jnp.float32,
        )


def solve_kernel(mp, zs, per_member, examples, other_ref, both_ref, u_ref, norm_ref, query_ref, out_ref):
    me = lax.axis_index("mp").astype(jnp.int32)
    half, columns = u_ref.shape[1:]
    chunk = query_ref.shape[3]
    scores = None
    for layer in range(2):
        square = jnp.zeros((4 * half, 4 * half), jnp.float32)
        mixed = jnp.zeros((2 * half, columns), jnp.float32)
        for k in range(mp):
            other = split_rows(other_ref, layer, (me ^ k) * (chunk // LANES), half, chunk)
            every = jnp.concatenate([both_ref[layer, :, k * chunk : (k + 1) * chunk], other], axis=0)
            square += contract_last(every, every)
            mixed += contract_last(other, query_ref[layer, k])
        gram = jnp.concatenate([fold_rows(square[: 2 * half]), fold_rows(square[2 * half :])], axis=0)
        own_u = u_ref[layer]
        other_u = fold_rows(mixed)
        u = jnp.concatenate([own_u, other_u], axis=0)
        u_high, u_low = split(jnp.concatenate([own_u, own_u, other_u, other_u], axis=0))
        gram_high, gram_low = split(gram)
        terms = jnp.dot(
            jnp.concatenate([gram_high, gram_low], axis=0), u_high, preferred_element_type=jnp.float32
        )
        ku = fold_rows(terms) + jnp.dot(gram_high, u_low, preferred_element_type=jnp.float32)
        qq = norm_ref[layer][:1]
        uu = jnp.sum(u * u, axis=0, keepdims=True)
        uku = jnp.sum(u * ku, axis=0, keepdims=True)
        step0 = qq / (uu / examples + damping * qq + epsilon)
        alpha = 1.0 - damping * step0
        beta = -step0 / examples
        rr = jnp.maximum(alpha * alpha * qq + 2.0 * alpha * beta * uu + beta * beta * uku, 0.0)
        a = alpha + rr / (qq + epsilon)
        sd = a * u + beta * ku
        dd = jnp.maximum(a * a * qq + 2.0 * a * beta * uu + beta * beta * uku, 0.0)
        step1 = rr / (jnp.sum(sd * sd, axis=0, keepdims=True) / examples + damping * dd + epsilon)

        value = [
            step0 * u[start : start + per_member] + step1 * sd[start : start + per_member]
            for start in range(0, half, zs * per_member)
        ]
        scores = value if scores is None else [total + part for total, part in zip(scores, value)]
    for place in range(mp):
        value = scores[0]
        for k in range(1, mp):
            value = jnp.where(me ^ k == place, scores[k], value)
        out_ref[place * per_member : (place + 1) * per_member, :] = value


def exchange(value, axis, count, unit=1):
    size = lax.axis_size(axis)
    found = [value]
    for k in range(1, count):
        found.append(lax.ppermute(value, axis, [(i, i ^ (k * unit)) for i in range(size)]))
    return found


def exchange_core(value, dp):
    return lax.ppermute(value, "dp", [(i, i ^ 1) for i in range(dp)])


def fast_device(
    token_ids,
    lengths,
    embed_grads,
    vocab_basis,
    embed_basis,
    layer_inputs,
    layer_grads,
    input_basis,
    output_basis,
    queries,
):
    vocab_rows, rank = vocab_basis.shape
    seq_count = lengths.shape[0]
    token_count, features = embed_grads.shape
    slot_len = token_count // seq_count
    mp, dp = lax.axis_size("mp"), lax.axis_size("dp")
    zs = dp // 2
    per_member = seq_count // mp
    examples = seq_count * dp
    placed = lambda space, *values: [pltpu.with_memory_space_constraint(v, space) for v in values]
    whole = lambda n: [pl.BlockSpec(memory_space=pltpu.VMEM)] * n
    limit = pltpu.CompilerParams(vmem_limit_bytes=16 * 2**20)

    block = per_member * slot_len
    sent = pl.pallas_call(
        functools.partial(project_kernel, vocab_rows, rank, slot_len, per_member),
        out_shape=[pltpu.VMEM((block, LANES), jnp.float32)] * mp,
        in_specs=[pl.BlockSpec(memory_space=pl.ANY)] * 9,
        out_specs=whole(mp),
        scratch_shapes=[
            pltpu.VMEM((seq_count, slot_len), jnp.int32),
            pltpu.SMEM((seq_count,), jnp.int32),
            pltpu.VMEM((rank, vocab_rows), jnp.bfloat16),
            pltpu.VMEM((3, token_count, features), jnp.bfloat16),
            pltpu.VMEM((3, LANES, features), jnp.bfloat16),
            pltpu.VMEM((seq_count, slot_len), jnp.int32),
            pltpu.SMEM((seq_count, slot_len), jnp.int32),
            pltpu.SemaphoreType.DMA((6,)),
            pltpu.SemaphoreType.DMA((3, mp)),
        ],
        compiler_params=limit,
        name="project",
    )(
        *placed(
            pltpu.HBM,
            token_ids.reshape(seq_count, slot_len),
            lengths,
            vocab_basis.T,
            embed_grads,
            layer_grads[0],
            layer_inputs[0],
            embed_basis.T,
            output_basis[0].T,
            input_basis[0].T,
        )
    )
    parts = [sent[0]]
    for k in range(1, mp):
        parts.append(lax.ppermute(sent[k], "mp", [(i, i ^ k) for i in range(mp)]))

    pieces = exchange(queries.transpose(0, 2, 1), "dp", zs, 2)
    rows = per_member * 2 * 8
    units = pl.pallas_call(
        functools.partial(sketch_kernel, rank, slot_len, per_member),
        out_shape=pltpu.VMEM((rows, LANES), jnp.float32),
        in_specs=whole(mp),
        out_specs=whole(1)[0],
        scratch_shapes=[pltpu.VMEM((per_member, 2 * rank, LANES), jnp.float32)],
        compiler_params=limit,
        name="sketch",
    )(*placed(pltpu.VMEM, *parts))
    along_z = jnp.concatenate(exchange(units, "dp", zs, 2))
    pieces = lax.optimization_barrier((*pieces, units))[:-1]
    qall = jnp.stack(exchange(jnp.stack(pieces), "mp", mp))
    qcore = exchange_core(qall, dp)
    mine = jnp.concatenate(exchange(along_z, "mp", mp))
    other = exchange_core(mine, dp)
    half = mp * zs * per_member
    columns = queries.shape[2] * dp
    sketch_len = rank * rank
    own_terms = pl.pallas_call(
        functools.partial(own_kernel, mp, zs),
        out_shape=[
            pltpu.VMEM((2, 2 * half, sketch_len), jnp.bfloat16),
            pltpu.VMEM((2, half, columns), jnp.float32),
            pltpu.VMEM((2, 8, columns), jnp.float32),
            pltpu.VMEM((2, mp, columns, queries.shape[1]), jnp.bfloat16),
        ],
        in_specs=whole(3),
        out_specs=whole(4),
        compiler_params=limit,
        name="own",
    )(*placed(pltpu.VMEM, mine, qall, qcore))
    return pl.pallas_call(
        functools.partial(solve_kernel, mp, zs, per_member, examples),
        out_shape=jax.ShapeDtypeStruct((seq_count, columns), jnp.float32),
        in_specs=whole(5),
        out_specs=whole(1)[0],
        compiler_params=limit,
        name="solve",
    )(*placed(pltpu.VMEM, other, *own_terms))


def power_of_two(n):
    return n & (n - 1) == 0


def solution(mesh):
    placed = (
        P("dp"),
        P("dp"),
        P("dp", "mp"),
        P("mp", None),
        P("mp", None),
        P(None, "dp", "mp"),
        P(None, "dp", "mp"),
        P(None, "mp", None),
        P(None, "mp", None),
        P(None, "mp", "dp"),
    )

    def per_device(*args):
        mp, dp = mesh.shape["mp"], mesh.shape["dp"]
        token_ids, lengths, layer_inputs, queries = args[0], args[1], args[5], args[9]
        seq_count, rank = lengths.shape[0], args[3].shape[1]
        fits = (
            layer_inputs.shape[0] == 1
            and token_ids.shape[0] == seq_count * LANES
            and rank * 4 == LANES
            and seq_count % 8 == 0
            and seq_count % mp == 0
            and power_of_two(mp)
            and power_of_two(dp)
            and dp % 2 == 0
            and queries.shape[1] % LANES == 0
            and queries.shape[2] % 16 == 0
            and queries.shape[2] * dp // 2 == LANES
        )
        if not fits:
            return general_device(*args)
        return fast_device(*args)

    return jax.shard_map(per_device, mesh=mesh, in_specs=placed, out_specs=P("dp", None), check_vma=False)
```

```python
import functools

import jax
import jax.numpy as jnp
from jax import lax
from jax.experimental import pallas as pl
from jax.experimental.pallas import tpu as pltpu
from jax.sharding import PartitionSpec as P


ITERS = 2
LANES = 128
AHEAD = 2

damping = 0.01
epsilon = 1e-06
highest = lax.Precision.HIGHEST


def solve_columns(right_side, apply_operator, column_norm, column_curve):
    solution = jnp.zeros_like(right_side)
    residual = right_side
    direction = right_side
    norm_now = column_norm(residual)
    for _ in range(ITERS):
        images = apply_operator(direction)
        step_size = norm_now / (column_curve(direction, images) + epsilon)
        solution = solution + step_size[:, None, :] * direction
        residual = residual - step_size[:, None, :] * images
        norm_next = column_norm(residual)
        direction = residual + (norm_next / (norm_now + epsilon))[:, None, :] * direction
        norm_now = norm_next
    return solution


def general_device(
    token_ids,
    lengths,
    embed_grads,
    vocab_basis,
    embed_basis,
    layer_inputs,
    layer_grads,
    input_basis,
    output_basis,
    queries,
):
    vocab_rows = vocab_basis.shape[0]
    basis_rank = embed_basis.shape[1]
    layer_count = layer_inputs.shape[0] + 1
    seq_count = lengths.shape[0]
    token_count = token_ids.shape[0]
    slot_len = token_count // seq_count
    sketch_len = basis_rank * basis_rank
    mp_index = lax.axis_index("mp")
    local_ids = token_ids - mp_index * vocab_rows
    inside = (local_ids >= 0) & (local_ids < vocab_rows)
    looked = jnp.take(vocab_basis, jnp.clip(local_ids, 0, vocab_rows - 1), axis=0)
    pieces = [
        jnp.dot(embed_grads, embed_basis, preferred_element_type=jnp.float32),
        jnp.where(inside[:, None], looked.astype(jnp.float32), 0.0),
    ]
    for layer in range(layer_count - 1):
        pieces.append(jnp.dot(layer_grads[layer], output_basis[layer], preferred_element_type=jnp.float32))
        pieces.append(jnp.dot(layer_inputs[layer], input_basis[layer], preferred_element_type=jnp.float32))
    projected = jnp.concatenate(pieces, axis=1)
    inverse_len = 1.0 / lengths.astype(jnp.float32)
    summed = lax.psum(projected, "mp")
    layout = summed.reshape(seq_count, slot_len, layer_count, 2, basis_rank)
    position = jnp.arange(slot_len, dtype=jnp.int32)
    weights = jnp.where(position[None, :] < lengths[:, None], inverse_len[:, None], 0.0)
    weighted = layout[:, :, :, 0, :] * weights[:, :, None, None]
    sketches = jnp.einsum(
        "stli,stlj->lsij", weighted, layout[:, :, :, 1, :], precision=highest
    ).reshape(layer_count, seq_count, sketch_len)
    examples = seq_count * lax.axis_size("dp")
    targets = lax.all_gather(queries, "dp", axis=2, tiled=True)
    everyone = lax.all_gather(sketches, "dp", axis=1, tiled=True)
    columns = lax.all_to_all(targets, "mp", split_axis=2, concat_axis=1, tiled=True)

    def apply_sketch(direction):
        inner_sums = jnp.einsum("lek,lkq->leq", everyone, direction, precision=highest)
        back_proj = jnp.einsum("lek,leq->lkq", everyone, inner_sums, precision=highest)
        return back_proj / examples + damping * direction

    def local_norm(residual):
        return jnp.sum(residual * residual, axis=1)

    def local_curve(direction, images):
        return jnp.sum(direction * images, axis=1)

    solution = solve_columns(columns.astype(jnp.float32), apply_sketch, local_norm, local_curve)
    partial_value = jnp.einsum("lek,lkq->eq", sketches, solution, precision=highest)
    return lax.all_gather(partial_value, "mp", axis=1, tiled=True)


def contract_last(left, right):
    return lax.dot_general(left, right, (((1,), (1,)), ((), ())), preferred_element_type=jnp.float32)


def project_kernel(
    vocab_rows,
    rank,
    slot_len,
    per_member,
    ids_any,
    len_any,
    table_any,
    grad0_any,
    grad1_any,
    input1_any,
    basis0_any,
    basis1_any,
    basis2_any,
    *refs,
):
    out_refs = refs[:-11]
    table_ref, own_ref, weight_ref, place_ref, share_ref, own_ids_ref = refs[-11:-5]
    ids_ref, len_ref, wide_ref, scalar_ref, sems = refs[-5:]
    small_sem, wide_sem = sems.at[pl.ds(0, 6)], sems.at[pl.ds(6, 3 * (len(out_refs) + 1))]
    members = len(out_refs) + 1
    me = lax.axis_index("mp").astype(jnp.int32)
    offset = me * vocab_rows
    main = vocab_rows // LANES
    block = per_member * slot_len

    def rows_of(r):
        return pl.ds(pl.multiple_of((me ^ r) * block, block), block)

    def wide_copy(k, r):
        source = (grad0_any, grad1_any, input1_any)[k]
        target = own_ref.at[k] if isinstance(r, int) and r == 0 else wide_ref.at[k, rows_of(r), :]
        return pltpu.make_async_copy(source.at[rows_of(r), :], target, wide_sem.at[k * members + r])

    ids_copy = pltpu.make_async_copy(ids_any, ids_ref, small_sem.at[0])
    len_copy = pltpu.make_async_copy(len_any, len_ref, small_sem.at[5])
    table_copy = pltpu.make_async_copy(table_any, table_ref, small_sem.at[1])
    basis_copies = [
        pltpu.make_async_copy(basis, weight_ref.at[k, pl.ds(k * rank, rank), :], small_sem.at[2 + k])
        for k, basis in enumerate((basis0_any, basis1_any, basis2_any))
    ]
    ids_copy.start()
    table_copy.start()
    len_copy.start()
    for copy in basis_copies:
        copy.start()
    for r in range(1, 1 + AHEAD):
        for k in range(3):
            wide_copy(k, r).start()
    for k in range(3):
        if k:
            weight_ref[k, : k * rank, :] = jnp.zeros((k * rank, weight_ref.shape[2]), jnp.bfloat16)
        weight_ref[k, (k + 1) * rank :, :] = jnp.zeros((LANES - (k + 1) * rank, weight_ref.shape[2]), jnp.bfloat16)
    ids_copy.wait()
    local = ids_ref[...] - offset
    position = lax.broadcasted_iota(jnp.int32, local.shape, 1)
    place_ref[...] = jnp.clip(local >> 7, 0, main - 1) * LANES + ((position - local) & (LANES - 1))
    scalar_copy = pltpu.make_async_copy(place_ref, scalar_ref, small_sem.at[0])
    scalar_copy.start()
    scalar_copy.wait()
    len_copy.wait()
    for copy in basis_copies:
        copy.wait()
    table_copy.wait()
    for r in [*range(1 + AHEAD, members), 0]:
        for k in range(3):
            wide_copy(k, r).start()

    def step(r, _):
        for k in range(3):
            wide_copy(k, r).wait()
        values = []
        for s in range(per_member):
            seq = (me ^ r) * per_member + s
            rows = pl.ds(pl.multiple_of(seq * slot_len, slot_len), slot_len)
            wide = [wide_ref[k, rows, :] for k in range(3)]
            found = look_up(scalar_ref, seq, ids_ref[pl.ds(seq, 1), :] - offset, table_ref, vocab_rows)
            position = lax.broadcasted_iota(jnp.int32, (slot_len, LANES), 0)
            values.append(combine(products(wide, weight_ref), found, shares(position, len_ref[seq])))
        for place, out_ref in enumerate(out_refs):

            @pl.when(r == place + 1)
            def _():
                for s in range(per_member):
                    out_ref[s * slot_len : (s + 1) * slot_len, :] = values[s]

        return 0

    lax.fori_loop(1, members, step, 0)
    for s in range(per_member):
        position = lax.broadcasted_iota(jnp.int32, (slot_len, LANES), 0)
        share_ref[s * slot_len : (s + 1) * slot_len, :] = shares(position, len_ref[me * per_member + s])
    own_ids_ref[...] = ids_ref[...] - offset
    for k in range(3):
        wide_copy(k, 0).wait()


def look_up(scalar_ref, seq, local, table_ref, vocab_rows):
    rank = table_ref.shape[0]
    main = vocab_rows // LANES
    tail = vocab_rows - main * LANES
    lane = lax.broadcasted_iota(jnp.int32, (rank, LANES), 1)
    found = jnp.zeros((rank, LANES), jnp.float32)
    for t in range(LANES):
        word = scalar_ref[seq, t]
        block = table_ref[:, pl.ds(pl.multiple_of(word & -LANES, LANES), LANES)].astype(jnp.float32)
        found = jnp.where(lane == t, pltpu.roll(block, word & (LANES - 1), 1), found)
    found = jnp.where((local >= 0) & (local < main * LANES), found, 0.0)
    if tail:
        sub = lax.broadcasted_iota(jnp.int32, (tail, LANES), 0)
        pick = jnp.where(local - main * LANES == sub, 1.0, 0.0).astype(jnp.bfloat16)
        found += jnp.dot(table_ref[:, main * LANES :], pick, preferred_element_type=jnp.float32)
    return found


def shares(position, live):
    return jnp.where(position < live, 1.0 / jnp.full(position.shape, live, jnp.int32).astype(jnp.float32), 0.0)


def products(wide, weight_ref):
    total = contract_last(wide[0], weight_ref[0])
    total += contract_last(wide[1], weight_ref[1])
    return total + contract_last(wide[2], weight_ref[2])


def combine(total, found, share):
    rank = found.shape[0]
    column = lax.broadcasted_iota(jnp.int32, total.shape, 1)
    spread = jnp.concatenate([jnp.zeros((3 * rank, LANES), jnp.float32), found], axis=0)
    return total * jnp.where(column < 2 * rank, share, 1.0) + spread.T


def own_block_kernel(
    vocab_rows,
    slot_len,
    per_member,
    table_ref,
    wide_ref,
    weight_ref,
    place_ref,
    share_ref,
    local_ref,
    out_ref,
    scalar_ref,
    copied,
):
    me = lax.axis_index("mp").astype(jnp.int32)
    copy = pltpu.make_async_copy(place_ref, scalar_ref, copied)
    copy.start()
    total = products([wide_ref[k] for k in range(3)], weight_ref)
    copy.wait()
    for s in range(per_member):
        seq = me * per_member + s
        rows = slice(s * slot_len, (s + 1) * slot_len)
        found = look_up(scalar_ref, seq, local_ref[pl.ds(seq, 1), :], table_ref, vocab_rows)
        out_ref[rows, :] = combine(total[rows], found, share_ref[rows, :])


def split(value):
    high = value.astype(jnp.bfloat16)
    return high, (value - high.astype(jnp.float32)).astype(jnp.bfloat16)


def fold_rows(value):
    half = value.shape[0] // 2
    return value[:half] + value[half:]


def sketch_kernel(rank, slot_len, per_member, *refs):
    parts, out_ref, full_ref = refs[:-2], refs[-2], refs[-1]
    lane = lax.broadcasted_iota(jnp.int32, (8, LANES), 1)
    for s in range(per_member):
        rows = slice(s * slot_len, (s + 1) * slot_len)
        total = parts[0][rows, :]
        for part in parts[1:]:
            total = total + part[rows, :]
        grads_high, grads_low = split(total[:, : 2 * rank])
        high, low = split(total)
        product = lax.dot_general(
            jnp.concatenate([grads_high, grads_low], axis=1),
            jnp.concatenate([high, low], axis=1),
            (((0,), (0,)), ((), ())),
            preferred_element_type=jnp.float32,
        )
        full_ref[s] = fold_rows(product[:, :LANES] + product[:, LANES:])
        for layer in range(2):
            source = 3 - layer
            unit = jnp.zeros((8, LANES), jnp.float32)
            for c in range(4):
                piece = full_ref[s, pl.ds(layer * rank + c, 8, stride=4), :]
                turned = pltpu.roll(piece, ((c - source) * rank) % LANES, 1)
                unit = jnp.where((lane >= c * rank) & (lane < (c + 1) * rank), turned, unit)
            out_ref[pl.ds((s * 2 + layer) * 8, 8), :] = unit


def split_rows(ref, layer, first, count, chunk):
    wide = [ref[pl.ds(layer * 8 + first + j, count, stride=16), :] for j in range(chunk // LANES)]
    return jnp.concatenate(split(jnp.concatenate(wide, axis=1)), axis=0)


def own_kernel(mp, zs, mine_ref, qmine_ref, qother_ref, both_ref, u_ref, norm_ref, query_ref):
    me = lax.axis_index("mp").astype(jnp.int32)
    mydp = lax.axis_index("dp").astype(jnp.int32)
    half, columns = u_ref.shape[1:]
    width, chunk = qmine_ref.shape[3:]
    for layer in range(2):
        mixed = jnp.zeros((2 * half, columns), jnp.float32)
        norms = jnp.zeros((columns, LANES), jnp.float32)
        for k in range(mp):
            both = split_rows(mine_ref, layer, (me ^ k) * (chunk // LANES), half, chunk)
            both_ref[layer, :, k * chunk : (k + 1) * chunk] = both
            for place in range(2 * zs):
                away = (mydp // 2) ^ (place // 2)
                query_ref[layer, k, place * width : (place + 1) * width, :] = jnp.where(
                    mydp % 2 == place % 2, qmine_ref[k, away, layer], qother_ref[k, away, layer]
                )
            query = query_ref[layer, k]
            mixed += contract_last(both, query)
            wide_query = query.astype(jnp.float32)
            squared = wide_query * wide_query
            for j in range(chunk // LANES):
                norms += squared[:, j * LANES : (j + 1) * LANES]
        u_ref[layer] = fold_rows(mixed)
        norm_ref[layer] = lax.dot_general(
            jnp.ones((8, LANES), jnp.float32),
            norms,
            (((1,), (1,)), ((), ())),
            precision=highest,
            preferred_element_type=jnp.float32,
        )


def solve_kernel(mp, zs, per_member, examples, other_ref, both_ref, u_ref, norm_ref, query_ref, out_ref):
    me = lax.axis_index("mp").astype(jnp.int32)
    half, columns = u_ref.shape[1:]
    chunk = query_ref.shape[3]
    scores = None
    for layer in range(2):
        square = jnp.zeros((4 * half, 4 * half), jnp.float32)
        mixed = jnp.zeros((2 * half, columns), jnp.float32)
        for k in range(mp):
            other = split_rows(other_ref, layer, (me ^ k) * (chunk // LANES), half, chunk)
            every = jnp.concatenate([both_ref[layer, :, k * chunk : (k + 1) * chunk], other], axis=0)
            square += contract_last(every, every)
            mixed += contract_last(other, query_ref[layer, k])
        gram = jnp.concatenate([fold_rows(square[: 2 * half]), fold_rows(square[2 * half :])], axis=0)
        own_u = u_ref[layer]
        other_u = fold_rows(mixed)
        u = jnp.concatenate([own_u, other_u], axis=0)
        u_high, u_low = split(jnp.concatenate([own_u, own_u, other_u, other_u], axis=0))
        gram_high, gram_low = split(gram)
        terms = jnp.dot(
            jnp.concatenate([gram_high, gram_low], axis=0), u_high, preferred_element_type=jnp.float32
        )
        ku = fold_rows(terms) + jnp.dot(gram_high, u_low, preferred_element_type=jnp.float32)
        qq = norm_ref[layer][:1]
        uu = jnp.sum(u * u, axis=0, keepdims=True)
        uku = jnp.sum(u * ku, axis=0, keepdims=True)
        step0 = qq / (uu / examples + damping * qq + epsilon)
        alpha = 1.0 - damping * step0
        beta = -step0 / examples
        rr = jnp.maximum(alpha * alpha * qq + 2.0 * alpha * beta * uu + beta * beta * uku, 0.0)
        a = alpha + rr / (qq + epsilon)
        sd = a * u + beta * ku
        dd = jnp.maximum(a * a * qq + 2.0 * a * beta * uu + beta * beta * uku, 0.0)
        step1 = rr / (jnp.sum(sd * sd, axis=0, keepdims=True) / examples + damping * dd + epsilon)

        value = [
            step0 * u[start : start + per_member] + step1 * sd[start : start + per_member]
            for start in range(0, half, zs * per_member)
        ]
        scores = value if scores is None else [total + part for total, part in zip(scores, value)]
    for place in range(mp):
        value = scores[0]
        for k in range(1, mp):
            value = jnp.where(me ^ k == place, scores[k], value)
        out_ref[place * per_member : (place + 1) * per_member, :] = value


def exchange(value, axis, count, unit=1):
    size = lax.axis_size(axis)
    found = [value]
    for k in range(1, count):
        found.append(lax.ppermute(value, axis, [(i, i ^ (k * unit)) for i in range(size)]))
    return found


def exchange_core(value, dp):
    return lax.ppermute(value, "dp", [(i, i ^ 1) for i in range(dp)])


def fast_device(
    token_ids,
    lengths,
    embed_grads,
    vocab_basis,
    embed_basis,
    layer_inputs,
    layer_grads,
    input_basis,
    output_basis,
    queries,
):
    vocab_rows, rank = vocab_basis.shape
    seq_count = lengths.shape[0]
    token_count, features = embed_grads.shape
    slot_len = token_count // seq_count
    mp, dp = lax.axis_size("mp"), lax.axis_size("dp")
    zs = dp // 2
    per_member = seq_count // mp
    examples = seq_count * dp
    placed = lambda space, *values: [pltpu.with_memory_space_constraint(v, space) for v in values]
    whole = lambda n: [pl.BlockSpec(memory_space=pltpu.VMEM)] * n
    limit = pltpu.CompilerParams(vmem_limit_bytes=16 * 2**20)

    block = per_member * slot_len
    sent = pl.pallas_call(
        functools.partial(project_kernel, vocab_rows, rank, slot_len, per_member),
        out_shape=[pltpu.VMEM((block, LANES), jnp.float32)] * (mp - 1)
        + [
            pltpu.VMEM((rank, vocab_rows), jnp.bfloat16),
            pltpu.VMEM((3, block, features), jnp.bfloat16),
            pltpu.VMEM((3, LANES, features), jnp.bfloat16),
            pltpu.VMEM((seq_count, slot_len), jnp.int32),
            pltpu.VMEM((block, LANES), jnp.float32),
            pltpu.VMEM((seq_count, slot_len), jnp.int32),
        ],
        in_specs=[pl.BlockSpec(memory_space=pl.ANY)] * 9,
        out_specs=whole(mp + 5),
        scratch_shapes=[
            pltpu.VMEM((seq_count, slot_len), jnp.int32),
            pltpu.SMEM((seq_count,), jnp.int32),
            pltpu.VMEM((3, token_count, features), jnp.bfloat16),
            pltpu.SMEM((seq_count, slot_len), jnp.int32),
            pltpu.SemaphoreType.DMA((6 + 3 * mp,)),
        ],
        compiler_params=limit,
        name="project",
    )(
        *placed(
            pltpu.HBM,
            token_ids.reshape(seq_count, slot_len),
            lengths,
            vocab_basis.T,
            embed_grads,
            layer_grads[0],
            layer_inputs[0],
            embed_basis.T,
            output_basis[0].T,
            input_basis[0].T,
        )
    )
    mine = pl.pallas_call(
        functools.partial(own_block_kernel, vocab_rows, slot_len, per_member),
        out_shape=pltpu.VMEM((block, LANES), jnp.float32),
        in_specs=whole(6),
        out_specs=whole(1)[0],
        scratch_shapes=[pltpu.SMEM((seq_count, slot_len), jnp.int32), pltpu.SemaphoreType.DMA],
        compiler_params=limit,
        name="own_block",
    )(*placed(pltpu.VMEM, *sent[mp - 1 :]))
    parts = [mine]
    for k in range(1, mp):
        parts.append(lax.ppermute(sent[k - 1], "mp", [(i, i ^ k) for i in range(mp)]))

    pieces = exchange(queries.transpose(0, 2, 1), "dp", zs, 2)
    rows = per_member * 2 * 8
    units = pl.pallas_call(
        functools.partial(sketch_kernel, rank, slot_len, per_member),
        out_shape=pltpu.VMEM((rows, LANES), jnp.float32),
        in_specs=whole(mp),
        out_specs=whole(1)[0],
        scratch_shapes=[pltpu.VMEM((per_member, 2 * rank, LANES), jnp.float32)],
        compiler_params=limit,
        name="sketch",
    )(*placed(pltpu.VMEM, *parts))
    along_z = jnp.concatenate(exchange(units, "dp", zs, 2))
    pieces = lax.optimization_barrier((*pieces, units))[:-1]
    qall = jnp.stack(exchange(jnp.stack(pieces), "mp", mp))
    qcore = exchange_core(qall, dp)
    mine = jnp.concatenate(exchange(along_z, "mp", mp))
    other = exchange_core(mine, dp)
    half = mp * zs * per_member
    columns = queries.shape[2] * dp
    sketch_len = rank * rank
    own_terms = pl.pallas_call(
        functools.partial(own_kernel, mp, zs),
        out_shape=[
            pltpu.VMEM((2, 2 * half, sketch_len), jnp.bfloat16),
            pltpu.VMEM((2, half, columns), jnp.float32),
            pltpu.VMEM((2, 8, columns), jnp.float32),
            pltpu.VMEM((2, mp, columns, queries.shape[1]), jnp.bfloat16),
        ],
        in_specs=whole(3),
        out_specs=whole(4),
        compiler_params=limit,
        name="own",
    )(*placed(pltpu.VMEM, mine, qall, qcore))
    return pl.pallas_call(
        functools.partial(solve_kernel, mp, zs, per_member, examples),
        out_shape=jax.ShapeDtypeStruct((seq_count, columns), jnp.float32),
        in_specs=whole(5),
        out_specs=whole(1)[0],
        compiler_params=limit,
        name="solve",
    )(*placed(pltpu.VMEM, other, *own_terms))


def power_of_two(n):
    return n & (n - 1) == 0


def solution(mesh):
    placed = (
        P("dp"),
        P("dp"),
        P("dp", "mp"),
        P("mp", None),
        P("mp", None),
        P(None, "dp", "mp"),
        P(None, "dp", "mp"),
        P(None, "mp", None),
        P(None, "mp", None),
        P(None, "mp", "dp"),
    )

    def per_device(*args):
        mp, dp = mesh.shape["mp"], mesh.shape["dp"]
        token_ids, lengths, layer_inputs, queries = args[0], args[1], args[5], args[9]
        seq_count, rank = lengths.shape[0], args[3].shape[1]
        fits = (
            layer_inputs.shape[0] == 1
            and token_ids.shape[0] == seq_count * LANES
            and rank * 4 == LANES
            and seq_count % 8 == 0
            and seq_count % mp == 0
            and power_of_two(mp)
            and power_of_two(dp)
            and dp % 2 == 0
            and queries.shape[1] % LANES == 0
            and queries.shape[2] % 16 == 0
            and queries.shape[2] * dp // 2 == LANES
        )
        if not fits:
            return general_device(*args)
        return fast_device(*args)

    return jax.shard_map(per_device, mesh=mesh, in_specs=placed, out_specs=P("dp", None), check_vma=False)
```

```python
import functools

import jax
import jax.numpy as jnp
from jax import lax
from jax.experimental import pallas as pl
from jax.experimental.pallas import tpu as pltpu
from jax.sharding import PartitionSpec as P


ITERS = 2
LANES = 128
AHEAD = 2

damping = 0.01
epsilon = 1e-06
highest = lax.Precision.HIGHEST


def solve_columns(right_side, apply_operator, column_norm, column_curve):
    solution = jnp.zeros_like(right_side)
    residual = right_side
    direction = right_side
    norm_now = column_norm(residual)
    for _ in range(ITERS):
        images = apply_operator(direction)
        step_size = norm_now / (column_curve(direction, images) + epsilon)
        solution = solution + step_size[:, None, :] * direction
        residual = residual - step_size[:, None, :] * images
        norm_next = column_norm(residual)
        direction = residual + (norm_next / (norm_now + epsilon))[:, None, :] * direction
        norm_now = norm_next
    return solution


def general_device(
    token_ids,
    lengths,
    embed_grads,
    vocab_basis,
    embed_basis,
    layer_inputs,
    layer_grads,
    input_basis,
    output_basis,
    queries,
):
    vocab_rows = vocab_basis.shape[0]
    basis_rank = embed_basis.shape[1]
    layer_count = layer_inputs.shape[0] + 1
    seq_count = lengths.shape[0]
    token_count = token_ids.shape[0]
    slot_len = token_count // seq_count
    sketch_len = basis_rank * basis_rank
    mp_index = lax.axis_index("mp")
    local_ids = token_ids - mp_index * vocab_rows
    inside = (local_ids >= 0) & (local_ids < vocab_rows)
    looked = jnp.take(vocab_basis, jnp.clip(local_ids, 0, vocab_rows - 1), axis=0)
    pieces = [
        jnp.dot(embed_grads, embed_basis, preferred_element_type=jnp.float32),
        jnp.where(inside[:, None], looked.astype(jnp.float32), 0.0),
    ]
    for layer in range(layer_count - 1):
        pieces.append(jnp.dot(layer_grads[layer], output_basis[layer], preferred_element_type=jnp.float32))
        pieces.append(jnp.dot(layer_inputs[layer], input_basis[layer], preferred_element_type=jnp.float32))
    projected = jnp.concatenate(pieces, axis=1)
    inverse_len = 1.0 / lengths.astype(jnp.float32)
    summed = lax.psum(projected, "mp")
    layout = summed.reshape(seq_count, slot_len, layer_count, 2, basis_rank)
    position = jnp.arange(slot_len, dtype=jnp.int32)
    weights = jnp.where(position[None, :] < lengths[:, None], inverse_len[:, None], 0.0)
    weighted = layout[:, :, :, 0, :] * weights[:, :, None, None]
    sketches = jnp.einsum(
        "stli,stlj->lsij", weighted, layout[:, :, :, 1, :], precision=highest
    ).reshape(layer_count, seq_count, sketch_len)
    examples = seq_count * lax.axis_size("dp")
    targets = lax.all_gather(queries, "dp", axis=2, tiled=True)
    everyone = lax.all_gather(sketches, "dp", axis=1, tiled=True)
    columns = lax.all_to_all(targets, "mp", split_axis=2, concat_axis=1, tiled=True)

    def apply_sketch(direction):
        inner_sums = jnp.einsum("lek,lkq->leq", everyone, direction, precision=highest)
        back_proj = jnp.einsum("lek,leq->lkq", everyone, inner_sums, precision=highest)
        return back_proj / examples + damping * direction

    def local_norm(residual):
        return jnp.sum(residual * residual, axis=1)

    def local_curve(direction, images):
        return jnp.sum(direction * images, axis=1)

    solution = solve_columns(columns.astype(jnp.float32), apply_sketch, local_norm, local_curve)
    partial_value = jnp.einsum("lek,lkq->eq", sketches, solution, precision=highest)
    return lax.all_gather(partial_value, "mp", axis=1, tiled=True)


def contract_last(left, right):
    return lax.dot_general(left, right, (((1,), (1,)), ((), ())), preferred_element_type=jnp.float32)


def project_kernel(
    vocab_rows,
    rank,
    slot_len,
    per_member,
    ids_any,
    len_any,
    table_any,
    grad0_any,
    grad1_any,
    input1_any,
    basis0_any,
    basis1_any,
    basis2_any,
    *refs,
):
    out_refs = refs[:-11]
    table_ref, own_ref, weight_ref, scalar_ref, share_ref, own_ids_ref = refs[-11:-5]
    ids_ref, len_ref, wide_ref, place_ref, sems = refs[-5:]
    small_sem, wide_sem = sems.at[pl.ds(0, 6)], sems.at[pl.ds(6, 3 * (len(out_refs) + 1))]
    members = len(out_refs) + 1
    me = lax.axis_index("mp").astype(jnp.int32)
    offset = me * vocab_rows
    main = vocab_rows // LANES
    block = per_member * slot_len

    def rows_of(r):
        return pl.ds(pl.multiple_of((me ^ r) * block, block), block)

    def wide_copy(k, r):
        source = (grad0_any, grad1_any, input1_any)[k]
        target = own_ref.at[k] if isinstance(r, int) and r == 0 else wide_ref.at[k, rows_of(r), :]
        return pltpu.make_async_copy(source.at[rows_of(r), :], target, wide_sem.at[k * members + r])

    ids_copy = pltpu.make_async_copy(ids_any, ids_ref, small_sem.at[0])
    len_copy = pltpu.make_async_copy(len_any, len_ref, small_sem.at[5])
    table_copy = pltpu.make_async_copy(table_any, table_ref, small_sem.at[1])
    basis_copies = [
        pltpu.make_async_copy(basis, weight_ref.at[k, pl.ds(k * rank, rank), :], small_sem.at[2 + k])
        for k, basis in enumerate((basis0_any, basis1_any, basis2_any))
    ]
    ids_copy.start()
    table_copy.start()
    len_copy.start()
    for copy in basis_copies:
        copy.start()
    for r in range(1, 1 + AHEAD):
        for k in range(3):
            wide_copy(k, r).start()
    for k in range(3):
        if k:
            weight_ref[k, : k * rank, :] = jnp.zeros((k * rank, weight_ref.shape[2]), jnp.bfloat16)
        weight_ref[k, (k + 1) * rank :, :] = jnp.zeros((LANES - (k + 1) * rank, weight_ref.shape[2]), jnp.bfloat16)
    ids_copy.wait()
    local = ids_ref[...] - offset
    position = lax.broadcasted_iota(jnp.int32, local.shape, 1)
    place_ref[...] = jnp.clip(local >> 7, 0, main - 1) * LANES + ((position - local) & (LANES - 1))
    scalar_copy = pltpu.make_async_copy(place_ref, scalar_ref, small_sem.at[0])
    scalar_copy.start()
    scalar_copy.wait()
    len_copy.wait()
    for copy in basis_copies:
        copy.wait()
    table_copy.wait()
    for r in [*range(1 + AHEAD, members), 0]:
        for k in range(3):
            wide_copy(k, r).start()

    def step(r, _):
        for k in range(3):
            wide_copy(k, r).wait()
        values = []
        for s in range(per_member):
            seq = (me ^ r) * per_member + s
            rows = pl.ds(pl.multiple_of(seq * slot_len, slot_len), slot_len)
            wide = [wide_ref[k, rows, :] for k in range(3)]
            found = look_up(scalar_ref, seq, ids_ref[pl.ds(seq, 1), :] - offset, table_ref, vocab_rows)
            position = lax.broadcasted_iota(jnp.int32, (slot_len, LANES), 0)
            values.append(combine(products(wide, weight_ref), found, shares(position, len_ref[seq])))
        for place, out_ref in enumerate(out_refs):

            @pl.when(r == place + 1)
            def _():
                for s in range(per_member):
                    out_ref[s * slot_len : (s + 1) * slot_len, :] = values[s]

        return 0

    lax.fori_loop(1, members, step, 0)
    for s in range(per_member):
        position = lax.broadcasted_iota(jnp.int32, (slot_len, LANES), 0)
        share_ref[s * slot_len : (s + 1) * slot_len, :] = shares(position, len_ref[me * per_member + s])
    own_ids_ref[...] = ids_ref[...] - offset
    for k in range(3):
        wide_copy(k, 0).wait()


def look_up(scalar_ref, seq, local, table_ref, vocab_rows):
    rank = table_ref.shape[0]
    main = vocab_rows // LANES
    tail = vocab_rows - main * LANES
    lane = lax.broadcasted_iota(jnp.int32, (rank, LANES), 1)
    found = jnp.zeros((rank, LANES), jnp.float32)
    for t in range(LANES):
        word = scalar_ref[seq, t]
        block = table_ref[:, pl.ds(pl.multiple_of(word & -LANES, LANES), LANES)].astype(jnp.float32)
        found = jnp.where(lane == t, pltpu.roll(block, word & (LANES - 1), 1), found)
    found = jnp.where((local >= 0) & (local < main * LANES), found, 0.0)
    if tail:
        sub = lax.broadcasted_iota(jnp.int32, (tail, LANES), 0)
        pick = jnp.where(local - main * LANES == sub, 1.0, 0.0).astype(jnp.bfloat16)
        found += jnp.dot(table_ref[:, main * LANES :], pick, preferred_element_type=jnp.float32)
    return found


def shares(position, live):
    return jnp.where(position < live, 1.0 / jnp.full(position.shape, live, jnp.int32).astype(jnp.float32), 0.0)


def products(wide, weight_ref):
    total = contract_last(wide[0], weight_ref[0])
    total += contract_last(wide[1], weight_ref[1])
    return total + contract_last(wide[2], weight_ref[2])


def combine(total, found, share):
    rank = found.shape[0]
    column = lax.broadcasted_iota(jnp.int32, total.shape, 1)
    spread = jnp.concatenate([jnp.zeros((3 * rank, LANES), jnp.float32), found], axis=0)
    return total * jnp.where(column < 2 * rank, share, 1.0) + spread.T


def own_block_kernel(
    vocab_rows,
    slot_len,
    per_member,
    table_ref,
    wide_ref,
    weight_ref,
    scalar_ref,
    share_ref,
    local_ref,
    out_ref,
):
    me = lax.axis_index("mp").astype(jnp.int32)
    total = products([wide_ref[k] for k in range(3)], weight_ref)
    for s in range(per_member):
        seq = me * per_member + s
        rows = slice(s * slot_len, (s + 1) * slot_len)
        found = look_up(scalar_ref, seq, local_ref[pl.ds(seq, 1), :], table_ref, vocab_rows)
        out_ref[rows, :] = combine(total[rows], found, share_ref[rows, :])


def split(value):
    high = value.astype(jnp.bfloat16)
    return high, (value - high.astype(jnp.float32)).astype(jnp.bfloat16)


def fold_rows(value):
    half = value.shape[0] // 2
    return value[:half] + value[half:]


def sketch_kernel(rank, slot_len, per_member, *refs):
    parts, out_ref, full_ref = refs[:-2], refs[-2], refs[-1]
    lane = lax.broadcasted_iota(jnp.int32, (8, LANES), 1)
    for s in range(per_member):
        rows = slice(s * slot_len, (s + 1) * slot_len)
        total = parts[0][rows, :]
        for part in parts[1:]:
            total = total + part[rows, :]
        grads_high, grads_low = split(total[:, : 2 * rank])
        high, low = split(total)
        product = lax.dot_general(
            jnp.concatenate([grads_high, grads_low], axis=1),
            jnp.concatenate([high, low], axis=1),
            (((0,), (0,)), ((), ())),
            preferred_element_type=jnp.float32,
        )
        full_ref[s] = fold_rows(product[:, :LANES] + product[:, LANES:])
        for layer in range(2):
            source = 3 - layer
            unit = jnp.zeros((8, LANES), jnp.float32)
            for c in range(4):
                piece = full_ref[s, pl.ds(layer * rank + c, 8, stride=4), :]
                turned = pltpu.roll(piece, ((c - source) * rank) % LANES, 1)
                unit = jnp.where((lane >= c * rank) & (lane < (c + 1) * rank), turned, unit)
            out_ref[pl.ds((s * 2 + layer) * 8, 8), :] = unit


def split_rows(ref, layer, first, count, chunk):
    wide = [ref[pl.ds(layer * 8 + first + j, count, stride=16), :] for j in range(chunk // LANES)]
    return jnp.concatenate(split(jnp.concatenate(wide, axis=1)), axis=0)


def own_kernel(mp, zs, mine_ref, qmine_ref, qother_ref, both_ref, u_ref, norm_ref, query_ref):
    me = lax.axis_index("mp").astype(jnp.int32)
    mydp = lax.axis_index("dp").astype(jnp.int32)
    half, columns = u_ref.shape[1:]
    width, chunk = qmine_ref.shape[3:]
    for layer in range(2):
        mixed = jnp.zeros((2 * half, columns), jnp.float32)
        norms = jnp.zeros((columns, LANES), jnp.float32)
        for k in range(mp):
            both = split_rows(mine_ref, layer, (me ^ k) * (chunk // LANES), half, chunk)
            both_ref[layer, :, k * chunk : (k + 1) * chunk] = both
            for place in range(2 * zs):
                away = (mydp // 2) ^ (place // 2)
                query_ref[layer, k, place * width : (place + 1) * width, :] = jnp.where(
                    mydp % 2 == place % 2, qmine_ref[k, away, layer], qother_ref[k, away, layer]
                )
            query = query_ref[layer, k]
            mixed += contract_last(both, query)
            wide_query = query.astype(jnp.float32)
            squared = wide_query * wide_query
            for j in range(chunk // LANES):
                norms += squared[:, j * LANES : (j + 1) * LANES]
        u_ref[layer] = fold_rows(mixed)
        norm_ref[layer] = lax.dot_general(
            jnp.ones((8, LANES), jnp.float32),
            norms,
            (((1,), (1,)), ((), ())),
            precision=highest,
            preferred_element_type=jnp.float32,
        )


def solve_kernel(mp, zs, per_member, examples, other_ref, both_ref, u_ref, norm_ref, query_ref, out_ref):
    me = lax.axis_index("mp").astype(jnp.int32)
    half, columns = u_ref.shape[1:]
    chunk = query_ref.shape[3]
    scores = None
    for layer in range(2):
        square = jnp.zeros((4 * half, 4 * half), jnp.float32)
        mixed = jnp.zeros((2 * half, columns), jnp.float32)
        for k in range(mp):
            other = split_rows(other_ref, layer, (me ^ k) * (chunk // LANES), half, chunk)
            every = jnp.concatenate([both_ref[layer, :, k * chunk : (k + 1) * chunk], other], axis=0)
            square += contract_last(every, every)
            mixed += contract_last(other, query_ref[layer, k])
        gram = jnp.concatenate([fold_rows(square[: 2 * half]), fold_rows(square[2 * half :])], axis=0)
        own_u = u_ref[layer]
        other_u = fold_rows(mixed)
        u = jnp.concatenate([own_u, other_u], axis=0)
        u_high, u_low = split(jnp.concatenate([own_u, own_u, other_u, other_u], axis=0))
        gram_high, gram_low = split(gram)
        terms = jnp.dot(
            jnp.concatenate([gram_high, gram_low], axis=0), u_high, preferred_element_type=jnp.float32
        )
        ku = fold_rows(terms) + jnp.dot(gram_high, u_low, preferred_element_type=jnp.float32)
        qq = norm_ref[layer][:1]
        uu = jnp.sum(u * u, axis=0, keepdims=True)
        uku = jnp.sum(u * ku, axis=0, keepdims=True)
        step0 = qq / (uu / examples + damping * qq + epsilon)
        alpha = 1.0 - damping * step0
        beta = -step0 / examples
        rr = jnp.maximum(alpha * alpha * qq + 2.0 * alpha * beta * uu + beta * beta * uku, 0.0)
        a = alpha + rr / (qq + epsilon)
        sd = a * u + beta * ku
        dd = jnp.maximum(a * a * qq + 2.0 * a * beta * uu + beta * beta * uku, 0.0)
        step1 = rr / (jnp.sum(sd * sd, axis=0, keepdims=True) / examples + damping * dd + epsilon)

        value = [
            step0 * u[start : start + per_member] + step1 * sd[start : start + per_member]
            for start in range(0, half, zs * per_member)
        ]
        scores = value if scores is None else [total + part for total, part in zip(scores, value)]
    for place in range(mp):
        value = scores[0]
        for k in range(1, mp):
            value = jnp.where(me ^ k == place, scores[k], value)
        out_ref[place * per_member : (place + 1) * per_member, :] = value


def exchange(value, axis, count, unit=1):
    size = lax.axis_size(axis)
    found = [value]
    for k in range(1, count):
        found.append(lax.ppermute(value, axis, [(i, i ^ (k * unit)) for i in range(size)]))
    return found


def exchange_core(value, dp):
    return lax.ppermute(value, "dp", [(i, i ^ 1) for i in range(dp)])


def fast_device(
    token_ids,
    lengths,
    embed_grads,
    vocab_basis,
    embed_basis,
    layer_inputs,
    layer_grads,
    input_basis,
    output_basis,
    queries,
):
    vocab_rows, rank = vocab_basis.shape
    seq_count = lengths.shape[0]
    token_count, features = embed_grads.shape
    slot_len = token_count // seq_count
    mp, dp = lax.axis_size("mp"), lax.axis_size("dp")
    zs = dp // 2
    per_member = seq_count // mp
    examples = seq_count * dp
    placed = lambda space, *values: [pltpu.with_memory_space_constraint(v, space) for v in values]
    whole = lambda n: [pl.BlockSpec(memory_space=pltpu.VMEM)] * n
    limit = pltpu.CompilerParams(vmem_limit_bytes=16 * 2**20)

    block = per_member * slot_len
    sent = pl.pallas_call(
        functools.partial(project_kernel, vocab_rows, rank, slot_len, per_member),
        out_shape=[pltpu.VMEM((block, LANES), jnp.float32)] * (mp - 1)
        + [
            pltpu.VMEM((rank, vocab_rows), jnp.bfloat16),
            pltpu.VMEM((3, block, features), jnp.bfloat16),
            pltpu.VMEM((3, LANES, features), jnp.bfloat16),
            pltpu.SMEM((seq_count, slot_len), jnp.int32),
            pltpu.VMEM((block, LANES), jnp.float32),
            pltpu.VMEM((seq_count, slot_len), jnp.int32),
        ],
        in_specs=[pl.BlockSpec(memory_space=pl.ANY)] * 9,
        out_specs=whole(mp + 2) + [pl.BlockSpec(memory_space=pltpu.SMEM)] + whole(2),
        scratch_shapes=[
            pltpu.VMEM((seq_count, slot_len), jnp.int32),
            pltpu.SMEM((seq_count,), jnp.int32),
            pltpu.VMEM((3, token_count, features), jnp.bfloat16),
            pltpu.VMEM((seq_count, slot_len), jnp.int32),
            pltpu.SemaphoreType.DMA((6 + 3 * mp,)),
        ],
        compiler_params=limit,
        name="project",
    )(
        *placed(
            pltpu.HBM,
            token_ids.reshape(seq_count, slot_len),
            lengths,
            vocab_basis.T,
            embed_grads,
            layer_grads[0],
            layer_inputs[0],
            embed_basis.T,
            output_basis[0].T,
            input_basis[0].T,
        )
    )
    mine = pl.pallas_call(
        functools.partial(own_block_kernel, vocab_rows, slot_len, per_member),
        out_shape=pltpu.VMEM((block, LANES), jnp.float32),
        in_specs=whole(3) + [pl.BlockSpec(memory_space=pltpu.SMEM)] + whole(2),
        out_specs=whole(1)[0],
        compiler_params=limit,
        name="own_block",
    )(
        *placed(pltpu.VMEM, *sent[mp - 1 : mp + 2]),
        *placed(pltpu.SMEM, sent[mp + 2]),
        *placed(pltpu.VMEM, *sent[mp + 3 :]),
    )
    parts = [mine]
    for k in range(1, mp):
        parts.append(lax.ppermute(sent[k - 1], "mp", [(i, i ^ k) for i in range(mp)]))

    pieces = exchange(queries.transpose(0, 2, 1), "dp", zs, 2)
    rows = per_member * 2 * 8
    units = pl.pallas_call(
        functools.partial(sketch_kernel, rank, slot_len, per_member),
        out_shape=pltpu.VMEM((rows, LANES), jnp.float32),
        in_specs=whole(mp),
        out_specs=whole(1)[0],
        scratch_shapes=[pltpu.VMEM((per_member, 2 * rank, LANES), jnp.float32)],
        compiler_params=limit,
        name="sketch",
    )(*placed(pltpu.VMEM, *parts))
    along_z = jnp.concatenate(exchange(units, "dp", zs, 2))
    pieces = lax.optimization_barrier((*pieces, units))[:-1]
    qall = jnp.stack(exchange(jnp.stack(pieces), "mp", mp))
    qcore = exchange_core(qall, dp)
    mine = jnp.concatenate(exchange(along_z, "mp", mp))
    other = exchange_core(mine, dp)
    half = mp * zs * per_member
    columns = queries.shape[2] * dp
    sketch_len = rank * rank
    own_terms = pl.pallas_call(
        functools.partial(own_kernel, mp, zs),
        out_shape=[
            pltpu.VMEM((2, 2 * half, sketch_len), jnp.bfloat16),
            pltpu.VMEM((2, half, columns), jnp.float32),
            pltpu.VMEM((2, 8, columns), jnp.float32),
            pltpu.VMEM((2, mp, columns, queries.shape[1]), jnp.bfloat16),
        ],
        in_specs=whole(3),
        out_specs=whole(4),
        compiler_params=limit,
        name="own",
    )(*placed(pltpu.VMEM, mine, qall, qcore))
    return pl.pallas_call(
        functools.partial(solve_kernel, mp, zs, per_member, examples),
        out_shape=jax.ShapeDtypeStruct((seq_count, columns), jnp.float32),
        in_specs=whole(5),
        out_specs=whole(1)[0],
        compiler_params=limit,
        name="solve",
    )(*placed(pltpu.VMEM, other, *own_terms))


def power_of_two(n):
    return n & (n - 1) == 0


def solution(mesh):
    placed = (
        P("dp"),
        P("dp"),
        P("dp", "mp"),
        P("mp", None),
        P("mp", None),
        P(None, "dp", "mp"),
        P(None, "dp", "mp"),
        P(None, "mp", None),
        P(None, "mp", None),
        P(None, "mp", "dp"),
    )

    def per_device(*args):
        mp, dp = mesh.shape["mp"], mesh.shape["dp"]
        token_ids, lengths, layer_inputs, queries = args[0], args[1], args[5], args[9]
        seq_count, rank = lengths.shape[0], args[3].shape[1]
        fits = (
            layer_inputs.shape[0] == 1
            and token_ids.shape[0] == seq_count * LANES
            and rank * 4 == LANES
            and seq_count % 8 == 0
            and seq_count % mp == 0
            and power_of_two(mp)
            and power_of_two(dp)
            and dp % 2 == 0
            and queries.shape[1] % LANES == 0
            and queries.shape[2] % 16 == 0
            and queries.shape[2] * dp // 2 == LANES
        )
        if not fits:
            return general_device(*args)
        return fast_device(*args)

    return jax.shard_map(per_device, mesh=mesh, in_specs=placed, out_specs=P("dp", None), check_vma=False)
```
